8 devices in a mesh: graph: 1 (over z), col: 2 (over y), row: 4 (over x, core).
Axes of the slice: x: 2, y: 2, z: 1, core: 2. Of those that a mesh axis runs over, the one named last changes fastest.
Arguments:
- flow_init: float32 [2048, 2048], P(('graph', 'row'), 'col')
- flow_graph: float32 [2048, 2048], P(('graph', 'row'), 'col')
Outputs:
- output: float32 [2048, 2048], P(('graph', 'row'), 'col')
All inputs are finite; a program needn't handle non-finite values.
Results may differ from the reference program's by a relative error of at most 0.001.
Values are sent between devices in bfloat16 or wider.
A program may use at most 1 GiB of HBM per device.

```python
import jax
import jax.numpy as jnp
from jax import lax

N = 2048
ITERATIONS = 3


def draw_flow(key, floor_level):
    key_width, key_noise = jax.random.split(key)
    node_index = jnp.arange(N, dtype=jnp.float32)
    band_width = N * jax.random.uniform(key_width, (N,), minval=0.01, maxval=0.15)
    raw_offset = jnp.abs(node_index[:, None] - node_index[None, :])
    cyclic_dist = jnp.minimum(raw_offset, N - raw_offset)
    noise_fac = jax.random.uniform(key_noise, (N, N), minval=0.5, maxval=1.5)
    weight = (floor_level + jnp.exp(-cyclic_dist / band_width[None, :])) * noise_fac
    return weight / jnp.sum(weight, axis=0, keepdims=True)


def setup_inputs(seed: int = 0, part: int = 0) -> dict:
    key = jax.random.fold_in(jax.random.key(seed), part)
    key_init, key_graph = jax.random.split(key)
    flow_init = N * draw_flow(key_init, 0.05)
    flow_graph = draw_flow(key_graph, 0.1)
    return {"flow_init": flow_init.astype(jnp.float32), "flow_graph": flow_graph.astype(jnp.float32)}


def reference(flow_init, flow_graph):
    graph_bf = flow_graph.astype(jnp.bfloat16)

    def iteration(flow_cur, unused):
        expanded = jnp.dot(flow_cur.astype(jnp.bfloat16), graph_bf, preferred_element_type=jnp.float32)
        inflated = expanded * expanded
        col_sum = jnp.sum(inflated, axis=0)
        return inflated * (N / col_sum), None

    flow_out, _ = lax.scan(iteration, flow_init, None, length=ITERATIONS)
    return flow_out
```

```python
import jax
import jax.numpy as jnp
from jax import lax
from jax.experimental import pallas as pl
from jax.experimental.pallas import tpu as pltpu
from jax.sharding import PartitionSpec as P

MESH = pl.DeviceIdType.MESH
BF16 = jnp.bfloat16
F32 = jnp.float32

ROWS = 512
COLS = 1024
ORDER = 2048
SUB = 64
NSUB = ROWS // SUB
KC = 256
NKC = COLS // KC


def mcl_kernel(a_hbm, g_hbm, m_ref, r_ref,
               a_f32, g_f32, G, A0, A1, A2, C1, C2, sums,
               ld_sem, gx_s, gx_r, gy_s, gy_r, dx_s, dx_r, ay_s, ay_r, cf_s, cf_r, ar_s, ar_r):
    graph, col, row = lax.axis_index("graph"), lax.axis_index("col"), lax.axis_index("row")
    x, core = row // 2, row % 2
    nb_x = (graph, col, (1 - x) * 2 + core)
    nb_y = (graph, 1 - col, row)
    nb_c = (graph, col, x * 2 + 1 - core)
    nb_xc = (graph, col, (1 - x) * 2 + 1 - core)

    half_own = lax.rem(x + col, 2)
    half_far = 1 - half_own

    def position(half, side, sub):
        n, s = sub // (128 // SUB), sub % (128 // SUB)
        return pl.multiple_of(half * COLS + KC * n + 128 * side + SUB * s, SUB)

    def remote(ref_src, ref_dst, send, recv, dev):
        return pltpu.make_async_remote_copy(src_ref=ref_src, dst_ref=ref_dst, send_sem=send, recv_sem=recv,
                                            device_id=dev, device_id_type=MESH)

    g_ld = [pltpu.make_async_copy(g_hbm.at[pl.ds(128 * i, 128)], g_f32.at[pl.ds(128 * i, 128)], ld_sem.at[i]) for i in range(4)]
    a_ld = pltpu.make_async_copy(a_hbm, a_f32, ld_sem.at[4])
    for cp in g_ld:
        cp.start()
    a_ld.start()

    barrier = pltpu.get_barrier_semaphore()
    for dev in (nb_x, nb_y, nb_c, nb_xc):
        pl.semaphore_signal(barrier, inc=1, device_id=dev, device_id_type=MESH)

    own_pos = [position(half_own, core, i) for i in range(NSUB)]
    own_at = [G.at[0, pl.ds(own_pos[i], SUB)] for i in range(NSUB)]
    gx_pos = [position(half_far, core, i) for i in range(NSUB)]
    gx_at = [G.at[0, pl.ds(gx_pos[i], SUB)] for i in range(NSUB)]
    gy_at = [G.at[1, pl.ds(own_pos[i], SUB)] for i in range(NSUB)]
    dx_at = [G.at[1, pl.ds(gx_pos[i], SUB)] for i in range(NSUB)]

    gx_cp = [remote(own_at[i], own_at[i], gx_s.at[i], gx_r.at[i], nb_x) for i in range(NSUB)]
    gy_cp = [remote(own_at[i], dx_at[i], gy_s.at[i], gy_r.at[i], nb_y) for i in range(NSUB)]
    dx_cp = [remote(gy_at[i], gy_at[i], dx_s.at[i], dx_r.at[i], nb_x) for i in range(NSUB)]
    cf_cp = [[remote(at[i], at[i], cf_s.at[k, i], cf_r.at[k, i], nb_c) for i in range(NSUB)]
             for k, at in enumerate((own_at, gx_at, gy_at, dx_at))]
    ay_cp = [remote(A0.at[:, pl.ds(KC * n, KC)], A0.at[:, pl.ds(COLS + KC * n, KC)], ay_s.at[n], ay_r.at[n], nb_y)
             for n in range(NKC)]

    def send_own(i):
        gx_cp[i].start()
        gy_cp[i].start()
        cf_cp[0][i].start()

    def put_columns(dst, half, src):
        for c in range(2):
            for n in range(4):
                b = 4 * c + n
                dst[:, half * COLS + KC * n + 128 * c:half * COLS + KC * n + 128 * c + 128] = src(b)

    for i in range(4):
        g_ld[i].wait()
        for s in range(128 // SUB):
            sub = i * (128 // SUB) + s
            G[0, pl.ds(own_pos[sub], SUB), :] = g_f32[SUB * sub:SUB * (sub + 1), :].astype(BF16)
        if i == 0:
            pl.semaphore_wait(barrier, 4)
        else:
            for s in range(128 // SUB):
                send_own((i - 1) * (128 // SUB) + s)
    a_ld.wait()
    put_columns(A0, 0, lambda b: a_f32[:, 128 * b:128 * b + 128].astype(BF16))
    for s in range(128 // SUB):
        send_own(3 * (128 // SUB) + s)

    def dot(a, g):
        return jnp.dot(a, g, preferred_element_type=F32)

    for i in range(NSUB):
        gx_cp[i].wait_recv()
        cf_cp[1][i].start()
        gy_cp[i].wait_recv()
        cf_cp[2][i].start()
        if i >= NSUB - 2:
            dx_cp[i - (NSUB - 2)].start()
            ay_cp[i - (NSUB - 2)].start()
        if i % 2 == 1 and i >= 3:
            n = i // 2 - 1
            for k in (0, 1):
                cf_cp[k][2 * n].wait_recv()
                cf_cp[k][2 * n + 1].wait_recv()
            d = dot(A0[:, KC * n:KC * n + KC], G[0, KC * n:KC * n + KC, :])
            if n == 0:
                C1[:, :COLS] = d
            else:
                C1[:, :COLS] += d
    n = NKC - 1
    for k in (0, 1):
        cf_cp[k][2 * n].wait_recv()
        cf_cp[k][2 * n + 1].wait_recv()
    C1[:, :COLS] += dot(A0[:, KC * n:KC * n + KC], G[0, KC * n:KC * n + KC, :])
    for i in range(NSUB):
        cf_cp[2][i].wait_recv()

    slots = []

    def share(it, lo, width, value, index):
        sums[it, 0, :, lo:lo + width] = value
        cps = []
        for r, dev in ((1, nb_c), (2, nb_x), (3, nb_xc)):
            cp = remote(sums.at[it, 0, :, pl.ds(lo, width)], sums.at[it, r, :, pl.ds(lo, width)],
                        ar_s.at[index, r - 1], ar_r.at[index, r - 1], dev)
            cp.start()
            cps.append(cp)
        slots.extend(cps)
        return it, lo, width, cps

    def gathered(handle):
        it, lo, width, cps = handle
        for cp in cps:
            cp.wait_recv()
        s = [sums[it, r, :, lo:lo + width] for r in range(4)]
        return float(ORDER) / ((s[0] + s[1]) + (s[2] + s[3]))

    def square_and_share(it, dst, lo, width, value, index):
        m = value * value
        dst[:, lo:lo + width] = m
        return share(it, lo, width, jnp.sum(m, axis=0, keepdims=True), index)

    near = None
    for n in range(NKC):
        for s in range(2):
            i = 2 * n + s
            dx_cp[i].wait_recv()
            cf_cp[3][i].start()
            if i + 2 < NSUB:
                dx_cp[i + 2].start()
        ay_cp[n].wait_recv()
        if n + 2 < NKC:
            ay_cp[n + 2].start()
        lo = KC * n
        hi = COLS + lo
        d0 = dot(A0[:, hi:hi + KC], G[0, hi:hi + KC, :])
        if n < NKC - 1:
            C1[:, :COLS] += d0
        else:
            near = square_and_share(0, C1, 0, COLS, C1[:, :COLS] + d0, 0)
        cf_cp[3][2 * n].wait_recv()
        cf_cp[3][2 * n + 1].wait_recv()
        d1 = dot(A0[:, lo:lo + KC], G[1, lo:lo + KC, :]) + dot(A0[:, hi:hi + KC], G[1, hi:hi + KC, :])
        if n == 0:
            C1[:, COLS:] = d1
        elif n < NKC - 1:
            C1[:, COLS:] += d1
        else:
            far = square_and_share(0, C1, COLS, COLS, C1[:, COLS:] + d1, 1)

    f = gathered(near)
    put_columns(A1, 0, lambda b: (C1[:, 128 * b:128 * b + 128] * f[:, 128 * b:128 * b + 128]).astype(BF16))
    for hc in range(2):
        C2[:, hc * COLS:(hc + 1) * COLS] = dot(A1[:, :COLS], G[hc, :COLS, :])
    f2 = gathered(far)
    put_columns(A1, 1, lambda b: (C1[:, COLS + 128 * b:COLS + 128 * b + 128] * f2[:, 128 * b:128 * b + 128]).astype(BF16))
    handles = []
    for hc in range(2):
        lo = hc * COLS
        handles.append(square_and_share(1, C2, lo, COLS, C2[:, lo:lo + COLS] + dot(A1[:, COLS:], G[hc, COLS:, :]), 2 + hc))

    for hc in range(2):
        fh = gathered(handles[hc])
        put_columns(A2, hc, lambda b: (C2[:, hc * COLS + 128 * b:hc * COLS + 128 * b + 128] * fh[:, 128 * b:128 * b + 128]).astype(BF16))
        d = dot(A2[:, hc * COLS:(hc + 1) * COLS], G[0, hc * COLS:(hc + 1) * COLS, :])
        if hc == 0:
            m_ref[...] = d
        else:
            last = square_and_share(2, m_ref, 0, COLS, m_ref[...] + d, 4)
    r_ref[...] = gathered(last)

    for cps in (gx_cp, gy_cp, dx_cp, ay_cp, *cf_cp, slots):
        for cp in cps:
            cp.wait_send()


def solution(mesh):
    block_spec = P(("graph", "row"), "col")

    def device_step(init_blk, graph_blk):
        dma = pltpu.SemaphoreType.DMA
        m, r = pl.pallas_call(
            mcl_kernel,
            name="mcl",
            out_shape=(jax.ShapeDtypeStruct((ROWS, COLS), F32), jax.ShapeDtypeStruct((1, COLS), F32)),
            in_specs=[pl.BlockSpec(memory_space=pl.ANY)] * 2,
            out_specs=(pl.BlockSpec(memory_space=pltpu.VMEM),) * 2,
            scratch_shapes=[
                pltpu.VMEM((ROWS, COLS), F32),
                pltpu.VMEM((ROWS, COLS), F32),
                pltpu.VMEM((2, ORDER, COLS), BF16),
                pltpu.VMEM((ROWS, ORDER), BF16),
                pltpu.VMEM((ROWS, ORDER), BF16),
                pltpu.VMEM((ROWS, ORDER), BF16),
                pltpu.VMEM((ROWS, ORDER), F32),
                pltpu.VMEM((ROWS, ORDER), F32),
                pltpu.VMEM((3, 4, 1, ORDER), F32),
                dma((5,)),
                dma((NSUB,)), dma((NSUB,)),
                dma((NSUB,)), dma((NSUB,)),
                dma((NSUB,)), dma((NSUB,)),
                dma((NKC,)), dma((NKC,)),
                dma((4, NSUB)), dma((4, NSUB)),
                dma((5, 3)), dma((5, 3)),
            ],
            compiler_params=pltpu.CompilerParams(collective_id=0, has_side_effects=True, vmem_limit_bytes=48 * 2**20),
        )(init_blk, graph_blk)
        return m * r

    return jax.shard_map(device_step, mesh=mesh, in_specs=(block_spec, block_spec), out_specs=block_spec, check_vma=False)
```

```python
import jax
import jax.numpy as jnp
from jax import lax
from jax.experimental import pallas as pl
from jax.experimental.pallas import tpu as pltpu
from jax.sharding import PartitionSpec as P

MESH = pl.DeviceIdType.MESH
BF16 = jnp.bfloat16
F32 = jnp.float32

ROWS = 512
COLS = 1024
ORDER = 2048
SUB = 64
NSUB = ROWS // SUB
KC = 256
NKC = COLS // KC
QW = COLS // 2


def place(b):
    return 2 * (b % 4) + b // 4


def mcl_kernel(a_hbm, g_hbm, m_ref, r_ref,
               a_f32, g_f32, G, A0, A1, A2, C1, C2, sums,
               ld_sem, gx_s, gx_r, gy_s, gy_r, dx_s, dx_r, ay_s, ay_r, cf_s, cf_r, ar_s, ar_r):
    graph, col, row = lax.axis_index("graph"), lax.axis_index("col"), lax.axis_index("row")
    x, core = row // 2, row % 2
    nb_x = (graph, col, (1 - x) * 2 + core)
    nb_y = (graph, 1 - col, row)
    nb_c = (graph, col, x * 2 + 1 - core)
    nb_xc = (graph, col, (1 - x) * 2 + 1 - core)

    half_own = lax.rem(x + col, 2)
    half_far = 1 - half_own

    def position(half, side, sub):
        n, s = sub // (128 // SUB), sub % (128 // SUB)
        return pl.multiple_of(half * COLS + KC * n + 128 * side + SUB * s, SUB)

    def remote(ref_src, ref_dst, send, recv, dev):
        return pltpu.make_async_remote_copy(src_ref=ref_src, dst_ref=ref_dst, send_sem=send, recv_sem=recv,
                                            device_id=dev, device_id_type=MESH)

    g_ld = [pltpu.make_async_copy(g_hbm.at[pl.ds(SUB * i, SUB)], g_f32.at[pl.ds(SUB * i, SUB)], ld_sem.at[i]) for i in range(NSUB)]
    a_ld = pltpu.make_async_copy(a_hbm, a_f32, ld_sem.at[NSUB])
    for cp in g_ld:
        cp.start()
    a_ld.start()

    barrier = pltpu.get_barrier_semaphore()
    for dev in (nb_x, nb_y, nb_c, nb_xc):
        pl.semaphore_signal(barrier, inc=1, device_id=dev, device_id_type=MESH)

    own_pos = [position(half_own, core, i) for i in range(NSUB)]
    own_at = [G.at[0, pl.ds(own_pos[i], SUB)] for i in range(NSUB)]
    gx_pos = [position(half_far, core, i) for i in range(NSUB)]
    gx_at = [G.at[0, pl.ds(gx_pos[i], SUB)] for i in range(NSUB)]
    gy_at = [G.at[1, pl.ds(own_pos[i], SUB)] for i in range(NSUB)]
    dx_at = [G.at[1, pl.ds(gx_pos[i], SUB)] for i in range(NSUB)]

    gx_cp = [remote(own_at[i], own_at[i], gx_s.at[i], gx_r.at[i], nb_x) for i in range(NSUB)]
    gy_cp = [remote(own_at[i], dx_at[i], gy_s.at[i], gy_r.at[i], nb_y) for i in range(NSUB)]
    dx_cp = [remote(gy_at[i], gy_at[i], dx_s.at[i], dx_r.at[i], nb_x) for i in range(NSUB)]
    cf_cp = [[remote(at[i], at[i], cf_s.at[k, i], cf_r.at[k, i], nb_c) for i in range(NSUB)]
             for k, at in enumerate((own_at, gx_at, gy_at, dx_at))]
    ay_cp = [remote(A0.at[:, pl.ds(KC * n, KC)], A0.at[:, pl.ds(COLS + KC * n, KC)], ay_s.at[n], ay_r.at[n], nb_y)
             for n in range(NKC)]

    def send_own(i):
        gx_cp[i].start()
        gy_cp[i].start()
        cf_cp[0][i].start()

    for i in range(NSUB):
        g_ld[i].wait()
        for b in range(8):
            p = place(b)
            G[0, pl.ds(own_pos[i], SUB), 128 * p:128 * p + 128] = g_f32[SUB * i:SUB * (i + 1), 128 * b:128 * b + 128].astype(BF16)
        if i == 0:
            pl.semaphore_wait(barrier, 4)
        else:
            send_own(i - 1)
    a_ld.wait()
    for b in range(8):
        p = place(b)
        A0[:, 128 * p:128 * p + 128] = a_f32[:, 128 * b:128 * b + 128].astype(BF16)
    send_own(NSUB - 1)

    def dot(a, g):
        return jnp.dot(a, g, preferred_element_type=F32)

    for i in range(NSUB):
        gx_cp[i].wait_recv()
        cf_cp[1][i].start()
        gy_cp[i].wait_recv()
        cf_cp[2][i].start()
        if i >= NSUB - 2:
            dx_cp[i - (NSUB - 2)].start()
            ay_cp[i - (NSUB - 2)].start()
        if i % 2 == 1 and i >= 3:
            n = i // 2 - 1
            for k in (0, 1):
                cf_cp[k][2 * n].wait_recv()
                cf_cp[k][2 * n + 1].wait_recv()
            d = dot(A0[:, KC * n:KC * n + KC], G[0, KC * n:KC * n + KC, :])
            if n == 0:
                C1[:, :COLS] = d
            else:
                C1[:, :COLS] += d
    n = NKC - 1
    for k in (0, 1):
        cf_cp[k][2 * n].wait_recv()
        cf_cp[k][2 * n + 1].wait_recv()
    C1[:, :COLS] += dot(A0[:, KC * n:KC * n + KC], G[0, KC * n:KC * n + KC, :])
    for i in range(NSUB):
        cf_cp[2][i].wait_recv()

    slots = []

    def share(it, lo, width, value):
        index = len(slots)
        sums[it, 0, :, lo:lo + width] = value
        cps = []
        for r, dev in ((1, nb_c), (2, nb_x), (3, nb_xc)):
            cp = remote(sums.at[it, 0, :, pl.ds(lo, width)], sums.at[it, r, :, pl.ds(lo, width)],
                        ar_s.at[index, r - 1], ar_r.at[index, r - 1], dev)
            cp.start()
            cps.append(cp)
        slots.append(cps)
        return it, lo, width, cps

    def gathered(handle):
        it, lo, width, cps = handle
        for cp in cps:
            cp.wait_recv()
        s = [sums[it, r, :, lo:lo + width] for r in range(4)]
        return float(ORDER) / ((s[0] + s[1]) + (s[2] + s[3]))

    def square_and_share(it, dst, lo, width, value):
        m = value * value
        dst[:, lo:lo + width] = m
        return share(it, lo, width, jnp.sum(m, axis=0, keepdims=True))

    def rescale(dst, src, q, handle):
        f = gathered(handle)
        dst[:, QW * q:QW * (q + 1)] = (src[:, QW * q:QW * (q + 1)] * f).astype(BF16)

    shared = []
    for n in range(NKC):
        for s in range(2):
            i = 2 * n + s
            dx_cp[i].wait_recv()
            cf_cp[3][i].start()
            if i + 2 < NSUB:
                dx_cp[i + 2].start()
        ay_cp[n].wait_recv()
        if n + 2 < NKC:
            ay_cp[n + 2].start()
        lo = KC * n
        hi = COLS + lo
        if n < NKC - 1:
            C1[:, :COLS] += dot(A0[:, hi:hi + KC], G[0, hi:hi + KC, :])
        else:
            for q in range(2):
                v = C1[:, QW * q:QW * (q + 1)] + dot(A0[:, hi:hi + KC], G[0, hi:hi + KC, QW * q:QW * (q + 1)])
                shared.append(square_and_share(0, C1, QW * q, QW, v))
        cf_cp[3][2 * n].wait_recv()
        cf_cp[3][2 * n + 1].wait_recv()
        for q in range(2):
            c = slice(QW * q, QW * (q + 1))
            d = dot(A0[:, lo:lo + KC], G[1, lo:lo + KC, c]) + dot(A0[:, hi:hi + KC], G[1, hi:hi + KC, c])
            at = slice(COLS + QW * q, COLS + QW * (q + 1))
            if n == 0:
                C1[:, at] = d
            elif n < NKC - 1:
                C1[:, at] += d
            else:
                shared.append(square_and_share(0, C1, COLS + QW * q, QW, C1[:, at] + d))

    rescale(A1, C1, 0, shared[0])
    for hc in range(2):
        C2[:, hc * COLS:(hc + 1) * COLS] = dot(A1[:, :QW], G[hc, :QW, :])
    for q in range(1, 4):
        rescale(A1, C1, q, shared[q])
    shared = []
    for q in range(4):
        c = slice(QW * q, QW * (q + 1))
        g = slice(QW * (q % 2), QW * (q % 2 + 1))
        shared.append(square_and_share(1, C2, QW * q, QW, C2[:, c] + dot(A1[:, QW:], G[q // 2, QW:, g])))

    for q in range(4):
        rescale(A2, C2, q, shared[q])
        d = dot(A2[:, QW * q:QW * (q + 1)], G[0, QW * q:QW * (q + 1), :])
        if q == 0:
            C1[:, :COLS] = d
        elif q < 3:
            C1[:, :COLS] += d
        else:
            v = C1[:, :COLS] + d
            m = v * v
            last = share(2, 0, COLS, jnp.sum(m, axis=0, keepdims=True))
            for b in range(8):
                p = place(b)
                m_ref[:, 128 * b:128 * b + 128] = m[:, 128 * p:128 * p + 128]
    f = gathered(last)
    for b in range(8):
        p = place(b)
        r_ref[:, 128 * b:128 * b + 128] = f[:, 128 * p:128 * p + 128]

    for cps in (gx_cp, gy_cp, dx_cp, ay_cp, *cf_cp, *slots):
        for cp in cps:
            cp.wait_send()


def solution(mesh):
    block_spec = P(("graph", "row"), "col")

    def device_step(init_blk, graph_blk):
        dma = pltpu.SemaphoreType.DMA
        in_hbm = [pltpu.with_memory_space_constraint(v, pltpu.HBM) for v in (init_blk, graph_blk)]
        m, r = pl.pallas_call(
            mcl_kernel,
            name="mcl",
            out_shape=(jax.ShapeDtypeStruct((ROWS, COLS), F32), jax.ShapeDtypeStruct((1, COLS), F32)),
            in_specs=[pl.BlockSpec(memory_space=pltpu.HBM)] * 2,
            out_specs=(pl.BlockSpec(memory_space=pltpu.VMEM),) * 2,
            scratch_shapes=[
                pltpu.VMEM((ROWS, COLS), F32),
                pltpu.VMEM((ROWS, COLS), F32),
                pltpu.VMEM((2, ORDER, COLS), BF16),
                pltpu.VMEM((ROWS, ORDER), BF16),
                pltpu.VMEM((ROWS, ORDER), BF16),
                pltpu.VMEM((ROWS, ORDER), BF16),
                pltpu.VMEM((ROWS, ORDER), F32),
                pltpu.VMEM((ROWS, ORDER), F32),
                pltpu.VMEM((3, 4, 1, ORDER), F32),
                dma((NSUB + 1,)),
                dma((NSUB,)), dma((NSUB,)),
                dma((NSUB,)), dma((NSUB,)),
                dma((NSUB,)), dma((NSUB,)),
                dma((NKC,)), dma((NKC,)),
                dma((4, NSUB)), dma((4, NSUB)),
                dma((9, 3)), dma((9, 3)),
            ],
            compiler_params=pltpu.CompilerParams(collective_id=0, has_side_effects=True, vmem_limit_bytes=48 * 2**20),
        )(*in_hbm)
        return m * r

    return jax.shard_map(device_step, mesh=mesh, in_specs=(block_spec, block_spec), out_specs=block_spec, check_vma=False)
```

```python
import jax
import jax.numpy as jnp
from jax import lax
from jax.experimental import pallas as pl
from jax.experimental.pallas import tpu as pltpu
from jax.sharding import PartitionSpec as P

MESH = pl.DeviceIdType.MESH
BF16 = jnp.bfloat16
F32 = jnp.float32

ROWS = 512
COLS = 1024
ORDER = 2048
SUB = 128
NSUB = ROWS // SUB
HALF = SUB // 2
TAIL = (NSUB - 1, NSUB - 0.5)
KC = 256
NKC = COLS // KC
PIECES_1 = ((0, 512), (512, 512), (1024, 512), (1536, 512))
PIECES_2 = ((0, 512), (512, 512), (1024, 512), (1536, 512))


def place(b):
    return 2 * (b % 4) + b // 4


def mcl_kernel(a_hbm, g_hbm, m_ref, r_ref,
               a_f32, g_f32, G, A0, A1, A2, C1, C2, sums,
               ld_sem, snd, gx_r, gy_r, dx_r, ay_r, c01_r, c2_r, c3_r, ar_s, ar_r):
    graph, col, row = lax.axis_index("graph"), lax.axis_index("col"), lax.axis_index("row")
    x, core = row // 2, row % 2
    nb_x = (graph, col, (1 - x) * 2 + core)
    nb_y = (graph, 1 - col, row)
    nb_c = (graph, col, x * 2 + 1 - core)
    nb_xc = (graph, col, (1 - x) * 2 + 1 - core)

    half_own = lax.rem(x + col, 2)
    half_far = 1 - half_own

    def position(half, side, sub):
        return pl.multiple_of(half * COLS + KC * (int(sub)) + SUB * side + int(SUB * (sub % 1)), HALF)

    def remote(ref_src, ref_dst, send, recv, dev):
        return pltpu.make_async_remote_copy(src_ref=ref_src, dst_ref=ref_dst, send_sem=send, recv_sem=recv,
                                            device_id=dev, device_id_type=MESH)

    loads = [pltpu.make_async_copy(src, dst, ld_sem.at[i]) for i, (src, dst) in enumerate((
        (g_hbm.at[pl.ds(0, SUB)], g_f32.at[pl.ds(0, SUB)]),
        (g_hbm.at[pl.ds(SUB, ROWS - SUB)], g_f32.at[pl.ds(SUB, ROWS - SUB)]),
        (a_hbm, a_f32)))]
    for cp in loads:
        cp.start()

    barrier = pltpu.get_barrier_semaphore()
    for dev in (nb_x, nb_y, nb_c, nb_xc):
        pl.semaphore_signal(barrier, inc=1, device_id=dev, device_id_type=MESH)

    def rows(hc, half, side, sub, n=SUB):
        return G.at[hc, pl.ds(position(half, side, sub), n)]

    own_at = [rows(0, half_own, core, i) for i in range(NSUB)]
    gx_at = [rows(0, half_far, core, i) for i in range(NSUB)]
    gy_at = [rows(1, half_own, core, i) for i in range(NSUB)]
    dx_at = [rows(1, half_far, core, i) for i in range(NSUB)]
    tail_y = [rows(1, half_own, core, i, HALF) for i in TAIL]
    tail_d = [rows(1, half_far, core, i, HALF) for i in TAIL]

    gx_cp = [remote(own_at[i], own_at[i], snd.at[0], gx_r.at[i], nb_x) for i in range(NSUB)]
    gy_cp = [remote(own_at[i], dx_at[i], snd.at[0], gy_r.at[i], nb_y) for i in range(NSUB)]
    dx_cp = [remote(at, at, snd.at[2], dx_r.at[i], nb_x) for i, at in enumerate(gy_at[:-1] + tail_y)]
    c0_cp = [remote(at, at, snd.at[0], c01_r.at[i], nb_c) for i, at in enumerate(own_at)]
    c1_cp = [remote(at, at, snd.at[1], c01_r.at[i], nb_c) for i, at in enumerate(gx_at)]
    c2_cp = [remote(at, at, snd.at[1], c2_r, nb_c) for at in gy_at]
    c3_cp = [remote(at, at, snd.at[3], c3_r.at[min(i, NSUB - 1)], nb_c) for i, at in enumerate(dx_at[:-1] + tail_d)]
    ay_cp = [remote(A0.at[:, pl.ds(KC * n, KC)], A0.at[:, pl.ds(COLS + KC * n, KC)], snd.at[2], ay_r.at[n], nb_y)
             for n in range(NKC)]

    def bytes_of(count, send, recv):
        at = G.at[0, pl.ds(0, count)] if count <= ORDER else G.at[:, pl.ds(0, count // 2)]
        return remote(at, at, send, recv, nb_c)

    def send_own(i):
        gx_cp[i].start()
        gy_cp[i].start()
        c0_cp[i].start()

    for i in range(NSUB):
        if i < 2:
            loads[i].wait()
        for b in range(8):
            p = place(b)
            G[0, pl.ds(position(half_own, core, i), SUB), 128 * p:128 * p + 128] = (
                g_f32[SUB * i:SUB * (i + 1), 128 * b:128 * b + 128].astype(BF16))
        if i == 0:
            pl.semaphore_wait(barrier, 4)
        else:
            send_own(i - 1)
    loads[2].wait()
    for b in range(8):
        p = place(b)
        A0[:, 128 * p:128 * p + 128] = a_f32[:, 128 * b:128 * b + 128].astype(BF16)
    send_own(NSUB - 1)

    def dot(a, g):
        return jnp.dot(a, g, preferred_element_type=F32)

    def near_step(n):
        bytes_of(2 * SUB, snd.at[0], c01_r.at[n]).wait_recv()
        d = dot(A0[:, KC * n:KC * n + KC], G[0, KC * n:KC * n + KC, :])
        if n == 0:
            C1[:, :COLS] = d
        else:
            C1[:, :COLS] += d

    for i in range(NSUB):
        gx_cp[i].wait_recv()
        c1_cp[i].start()
        gy_cp[i].wait_recv()
        c2_cp[i].start()
        if i == NSUB - 2:
            dx_cp[0].start()
            ay_cp[0].start()
        if i >= 1:
            near_step(i - 1)
    dx_cp[1].start()
    ay_cp[1].start()
    near_step(NSUB - 1)
    bytes_of(ROWS, snd.at[1], c2_r).wait_recv()

    slots = []

    def share(it, lo, width, value):
        index = len(slots)
        slots.append(index)
        sums[it, 0, :, lo:lo + width] = value
        for r, dev in ((1, nb_c), (2, nb_x), (3, nb_xc)):
            remote(sums.at[it, 0, :, pl.ds(lo, width)], sums.at[it, r, :, pl.ds(lo, width)],
                   ar_s.at[it], ar_r.at[index], dev).start()
        return it, lo, width, index

    def three(it, lo, width, index):
        at = sums.at[it, pl.ds(1, 3), :, pl.ds(lo, width)]
        return remote(at, at, ar_s.at[it], ar_r.at[index], nb_c)

    def gathered(handle):
        it, lo, width, index = handle
        three(it, lo, width, index).wait_recv()
        s = [sums[it, r, :, lo:lo + width] for r in range(4)]
        return float(ORDER) / ((s[0] + s[1]) + (s[2] + s[3]))

    def square_and_share(it, dst, lo, width, value):
        m = value * value
        dst[:, lo:lo + width] = m
        return share(it, lo, width, jnp.sum(m, axis=0, keepdims=True))

    def rescale(dst, src, handle):
        f = gathered(handle)
        lo, width = handle[1:3]
        dst[:, lo:lo + width] = (src[:, lo:lo + width] * f).astype(BF16)

    def graph(lo, depth, first, width):
        return G[first // COLS, lo:lo + depth, first % COLS:first % COLS + width]

    shared = []
    for n in range(NKC):
        if n == 0:
            bytes_of(3 * ROWS, snd.at[0], c2_r).wait_send()
        for i in (n,) if n < NSUB - 1 else (n, n + 1):
            dx_cp[i].wait_recv()
            c3_cp[i].start()
            if i + 2 < len(dx_cp):
                dx_cp[i + 2].start()
            if i == n == 2:
                bytes_of(2 * ROWS, snd.at[1], c2_r).wait_send()
        ay_cp[n].wait_recv()
        if n + 2 < NKC:
            ay_cp[n + 2].start()
        lo = KC * n
        hi = COLS + lo
        if n < NKC - 1:
            C1[:, :COLS] += dot(A0[:, hi:hi + KC], G[0, hi:hi + KC, :])
        else:
            for first, width in PIECES_1:
                if first < COLS:
                    v = C1[:, first:first + width] + dot(A0[:, hi:hi + KC], graph(hi, KC, first, width))
                    shared.append(square_and_share(0, C1, first, width, v))
        bytes_of(SUB, snd.at[3], c3_r.at[n]).wait_recv()
        for first, width in PIECES_1:
            if first < COLS:
                continue
            d = dot(A0[:, lo:lo + KC], graph(lo, KC, first, width)) + dot(A0[:, hi:hi + KC], graph(hi, KC, first, width))
            if n == 0:
                C1[:, first:first + width] = d
            elif n < NKC - 1:
                C1[:, first:first + width] += d
            else:
                shared.append(square_and_share(0, C1, first, width, C1[:, first:first + width] + d))

    bytes_of(2 * ROWS, snd.at[2], c2_r).wait_send()
    bytes_of(ROWS, snd.at[3], c2_r).wait_send()
    done = 0
    for t in range(1):
        rescale(A1, C1, shared[t])
        lo, depth = PIECES_1[t]
        for hc in range(2):
            at = slice(hc * COLS, (hc + 1) * COLS)
            d = dot(A1[:, lo:lo + depth], G[hc, lo:lo + depth, :])
            if t == 0:
                C2[:, at] = d
            else:
                C2[:, at] += d
        done = lo + depth
    for handle in shared[1:]:
        rescale(A1, C1, handle)
    three(0, 0, ORDER, 0).wait_send()
    shared = []
    for first, width in PIECES_2:
        v = C2[:, first:first + width] + dot(A1[:, done:], graph(done, ORDER - done, first, width))
        shared.append(square_and_share(1, C2, first, width, v))

    for t, (lo, depth) in enumerate(PIECES_2):
        rescale(A2, C2, shared[t])
        d = dot(A2[:, lo:lo + depth], G[0, lo:lo + depth, :])
        if t == 0:
            C1[:, :COLS] = d
        elif t < len(PIECES_2) - 1:
            C1[:, :COLS] += d
        else:
            v = C1[:, :COLS] + d
            m = v * v
            last = share(2, 0, COLS, jnp.sum(m, axis=0, keepdims=True))
            for b in range(8):
                p = place(b)
                m_ref[:, 128 * b:128 * b + 128] = m[:, 128 * p:128 * p + 128]
    three(1, 0, ORDER, 0).wait_send()
    f = gathered(last)
    for b in range(8):
        p = place(b)
        r_ref[:, 128 * b:128 * b + 128] = f[:, 128 * p:128 * p + 128]
    three(2, 0, COLS, 0).wait_send()


def scale_kernel(m_ref, r_ref, out_hbm, out, sem):
    factor = r_ref[...]
    step = ROWS // 8
    for i in range(8):
        at = pl.ds(step * i, step)
        out[at, :] = m_ref[at, :] * factor
        pltpu.make_async_copy(out.at[at], out_hbm.at[at], sem).start()
    pltpu.make_async_copy(out, out_hbm, sem).wait()


def solution(mesh):
    block_spec = P(("graph", "row"), "col")

    def device_step(init_blk, graph_blk):
        dma = pltpu.SemaphoreType.DMA
        in_hbm = [pltpu.with_memory_space_constraint(v, pltpu.HBM) for v in (init_blk, graph_blk)]
        m, r = pl.pallas_call(
            mcl_kernel,
            name="mcl",
            out_shape=(jax.ShapeDtypeStruct((ROWS, COLS), F32), jax.ShapeDtypeStruct((1, COLS), F32)),
            in_specs=[pl.BlockSpec(memory_space=pltpu.HBM)] * 2,
            out_specs=(pl.BlockSpec(memory_space=pltpu.VMEM),) * 2,
            scratch_shapes=[
                pltpu.VMEM((ROWS, COLS), F32),
                pltpu.VMEM((ROWS, COLS), F32),
                pltpu.VMEM((2, ORDER, COLS), BF16),
                pltpu.VMEM((ROWS, ORDER), BF16),
                pltpu.VMEM((ROWS, ORDER), BF16),
                pltpu.VMEM((ROWS, ORDER), BF16),
                pltpu.VMEM((ROWS, ORDER), F32),
                pltpu.VMEM((ROWS, ORDER), F32),
                pltpu.VMEM((3, 4, 1, ORDER), F32),
                dma((3,)), dma((4,)),
                dma((NSUB,)), dma((NSUB,)), dma((NSUB + 1,)), dma((NKC,)),
                dma((NSUB,)), dma(()), dma((NSUB,)),
                dma((3,)), dma((len(PIECES_1) + len(PIECES_2) + 1,)),
            ],
            compiler_params=pltpu.CompilerParams(collective_id=0, has_side_effects=True, vmem_limit_bytes=48 * 2**20),
        )(*in_hbm)
        return pl.pallas_call(
            scale_kernel,
            name="scale",
            out_shape=jax.ShapeDtypeStruct((ROWS, COLS), F32),
            in_specs=[pl.BlockSpec(memory_space=pltpu.VMEM)] * 2,
            out_specs=pl.BlockSpec(memory_space=pltpu.HBM),
            scratch_shapes=[pltpu.VMEM((ROWS, COLS), F32), dma(())],
            compiler_params=pltpu.CompilerParams(vmem_limit_bytes=8 * 2**20),
        )(m, r)

    return jax.shard_map(device_step, mesh=mesh, in_specs=(block_spec, block_spec), out_specs=block_spec, check_vma=False)
```

```python
import jax
import jax.numpy as jnp
from jax import lax
from jax.experimental import pallas as pl
from jax.experimental.pallas import tpu as pltpu
from jax.sharding import PartitionSpec as P

MESH = pl.DeviceIdType.MESH
BF16 = jnp.bfloat16
F32 = jnp.float32

ROWS = 512
COLS = 1024
ORDER = 2048
SUB = 128
NSUB = ROWS // SUB
HALF = SUB // 2
TAIL = (NSUB - 1, NSUB - 0.5)
KC = 256
NKC = COLS // KC
PIECES_1 = ((0, 512), (512, 512), (1024, 1024))
PIECES_2 = ((1024, 512), (1536, 512), (0, 512), (512, 512))


def place(b):
    return 2 * (b % 4) + b // 4


def mcl_kernel(a_hbm, g_hbm, m_ref, r_ref,
               a_f32, g_f32, G, A0, A1, A2, C1, C2, sums,
               ld_sem, snd, gx_r, gy_r, dx_r, ay_r, c01_r, c2_r, c3_r, ar_s, ar_r):
    graph, col, row = lax.axis_index("graph"), lax.axis_index("col"), lax.axis_index("row")
    x, core = row // 2, row % 2
    nb_x = (graph, col, (1 - x) * 2 + core)
    nb_y = (graph, 1 - col, row)
    nb_c = (graph, col, x * 2 + 1 - core)
    nb_xc = (graph, col, (1 - x) * 2 + 1 - core)

    half_own = lax.rem(x + col, 2)
    half_far = 1 - half_own

    def position(half, side, sub):
        return pl.multiple_of(half * COLS + KC * (int(sub)) + SUB * side + int(SUB * (sub % 1)), HALF)

    def remote(ref_src, ref_dst, send, recv, dev):
        return pltpu.make_async_remote_copy(src_ref=ref_src, dst_ref=ref_dst, send_sem=send, recv_sem=recv,
                                            device_id=dev, device_id_type=MESH)

    loads = [pltpu.make_async_copy(src, dst, ld_sem.at[i]) for i, (src, dst) in enumerate((
        (g_hbm.at[pl.ds(0, SUB)], g_f32.at[pl.ds(0, SUB)]),
        (g_hbm.at[pl.ds(SUB, ROWS - SUB)], g_f32.at[pl.ds(SUB, ROWS - SUB)]),
        (a_hbm, a_f32)))]
    for cp in loads:
        cp.start()

    barrier = pltpu.get_barrier_semaphore()
    for dev in (nb_x, nb_y, nb_c, nb_xc):
        pl.semaphore_signal(barrier, inc=1, device_id=dev, device_id_type=MESH)

    def rows(hc, half, side, sub, n=SUB):
        return G.at[hc, pl.ds(position(half, side, sub), n)]

    own_at = [rows(0, half_own, core, i) for i in range(NSUB)]
    gx_at = [rows(0, half_far, core, i) for i in range(NSUB)]
    gy_at = [rows(1, half_own, core, i) for i in range(NSUB)]
    dx_at = [rows(1, half_far, core, i) for i in range(NSUB)]
    tail_y = [rows(1, half_own, core, i, HALF) for i in TAIL]
    tail_d = [rows(1, half_far, core, i, HALF) for i in TAIL]

    gx_cp = [remote(own_at[i], own_at[i], snd.at[0], gx_r.at[i], nb_x) for i in range(NSUB)]
    gy_cp = [remote(own_at[i], dx_at[i], snd.at[0], gy_r.at[i], nb_y) for i in range(NSUB)]
    dx_cp = [remote(at, at, snd.at[2], dx_r.at[i], nb_x) for i, at in enumerate(gy_at[:-1] + tail_y)]
    c0_cp = [remote(at, at, snd.at[0], c01_r.at[i], nb_c) for i, at in enumerate(own_at)]
    c1_cp = [remote(at, at, snd.at[1], c01_r.at[i], nb_c) for i, at in enumerate(gx_at)]
    c2_cp = [remote(at, at, snd.at[1], c2_r, nb_c) for at in gy_at]
    c3_cp = [remote(at, at, snd.at[3], c3_r.at[min(i, NSUB - 1)], nb_c) for i, at in enumerate(dx_at[:-1] + tail_d)]
    ay_cp = [remote(A0.at[:, pl.ds(KC * n, KC)], A0.at[:, pl.ds(COLS + KC * n, KC)], snd.at[2], ay_r.at[n], nb_y)
             for n in range(NKC)]

    def bytes_of(count, send, recv):
        at = G.at[0, pl.ds(0, count)] if count <= ORDER else G.at[:, pl.ds(0, count // 2)]
        return remote(at, at, send, recv, nb_c)

    def send_own(i):
        gx_cp[i].start()
        gy_cp[i].start()
        c0_cp[i].start()

    for i in range(NSUB):
        if i < 2:
            loads[i].wait()
        for b in range(8):
            p = place(b)
            G[0, pl.ds(position(half_own, core, i), SUB), 128 * p:128 * p + 128] = (
                g_f32[SUB * i:SUB * (i + 1), 128 * b:128 * b + 128].astype(BF16))
        if i == 0:
            pl.semaphore_wait(barrier, 4)
        else:
            send_own(i - 1)
    loads[2].wait()
    for b in range(8):
        p = place(b)
        A0[:, 128 * p:128 * p + 128] = a_f32[:, 128 * b:128 * b + 128].astype(BF16)
    send_own(NSUB - 1)

    def dot(a, g):
        return jnp.dot(a, g, preferred_element_type=F32)

    def near_step(n):
        bytes_of(2 * SUB, snd.at[0], c01_r.at[n]).wait_recv()
        d = dot(A0[:, KC * n:KC * n + KC], G[0, KC * n:KC * n + KC, :])
        if n == 0:
            C1[:, :COLS] = d
        else:
            C1[:, :COLS] += d

    for i in range(NSUB):
        gx_cp[i].wait_recv()
        c1_cp[i].start()
        gy_cp[i].wait_recv()
        c2_cp[i].start()
        if i == NSUB - 2:
            dx_cp[0].start()
            ay_cp[0].start()
        if i >= 1:
            near_step(i - 1)
    dx_cp[1].start()
    ay_cp[1].start()
    near_step(NSUB - 1)
    bytes_of(ROWS, snd.at[1], c2_r).wait_recv()

    slots = []

    def share(it, lo, width, value):
        index = len(slots)
        slots.append(index)
        sums[it, 0, :, lo:lo + width] = value
        for r, dev in ((1, nb_c), (2, nb_x), (3, nb_xc)):
            remote(sums.at[it, 0, :, pl.ds(lo, width)], sums.at[it, r, :, pl.ds(lo, width)],
                   ar_s.at[it], ar_r.at[index], dev).start()
        return it, lo, width, index

    def three(it, lo, width, index):
        at = sums.at[it, pl.ds(1, 3), :, pl.ds(lo, width)]
        return remote(at, at, ar_s.at[it], ar_r.at[index], nb_c)

    def gathered(handle):
        it, lo, width, index = handle
        three(it, lo, width, index).wait_recv()
        s = [sums[it, r, :, lo:lo + width] for r in range(4)]
        return float(ORDER) / ((s[0] + s[1]) + (s[2] + s[3]))

    def square_and_share(it, dst, lo, width, value):
        m = value * value
        dst[:, lo:lo + width] = m
        return share(it, lo, width, jnp.sum(m, axis=0, keepdims=True))

    def rescale(dst, src, handle):
        f = gathered(handle)
        lo, width = handle[1:3]
        dst[:, lo:lo + width] = (src[:, lo:lo + width] * f).astype(BF16)

    def graph(lo, depth, first, width):
        return G[first // COLS, lo:lo + depth, first % COLS:first % COLS + width]

    shared = []
    for n in range(NKC):
        if n == 0:
            bytes_of(3 * ROWS, snd.at[0], c2_r).wait_send()
        for i in (n,) if n < NSUB - 1 else (n, n + 1):
            dx_cp[i].wait_recv()
            c3_cp[i].start()
            if i + 2 < len(dx_cp):
                dx_cp[i + 2].start()
            if i == n == 2:
                bytes_of(2 * ROWS, snd.at[1], c2_r).wait_send()
        ay_cp[n].wait_recv()
        if n + 2 < NKC:
            ay_cp[n + 2].start()
        lo = KC * n
        hi = COLS + lo
        if n < NKC - 1:
            C1[:, :COLS] += dot(A0[:, hi:hi + KC], G[0, hi:hi + KC, :])
        else:
            for first, width in PIECES_1:
                if first < COLS:
                    v = C1[:, first:first + width] + dot(A0[:, hi:hi + KC], graph(hi, KC, first, width))
                    shared.append(square_and_share(0, C1, first, width, v))
        bytes_of(SUB, snd.at[3], c3_r.at[n]).wait_recv()
        for first, width in PIECES_1:
            if first < COLS:
                continue
            d = dot(A0[:, lo:lo + KC], graph(lo, KC, first, width)) + dot(A0[:, hi:hi + KC], graph(hi, KC, first, width))
            if n == 0:
                C1[:, first:first + width] = d
            elif n < NKC - 1:
                C1[:, first:first + width] += d
            else:
                shared.append(square_and_share(0, C1, first, width, C1[:, first:first + width] + d))

    bytes_of(2 * ROWS, snd.at[2], c2_r).wait_send()
    bytes_of(ROWS, snd.at[3], c2_r).wait_send()
    done = 0
    for t in range(1):
        rescale(A1, C1, shared[t])
        lo, depth = PIECES_1[t]
        for hc in range(2):
            at = slice(hc * COLS, (hc + 1) * COLS)
            d = dot(A1[:, lo:lo + depth], G[hc, lo:lo + depth, :])
            if t == 0:
                C2[:, at] = d
            else:
                C2[:, at] += d
        done = lo + depth
    factors = [gathered(handle) for handle in shared[1:]]
    three(0, 0, ORDER, 0).wait_send()
    shared = []
    held = None
    for first, width in PIECES_2:
        v = C2[:, first:first + width]
        for (lo, depth), f in zip(PIECES_1[1:], factors):
            if first == PIECES_2[0][0]:
                A1[:, lo:lo + depth] = (C1[:, lo:lo + depth] * f).astype(BF16)
            v += dot(A1[:, lo:lo + depth], graph(lo, depth, first, width))
            if held is not None:
                shared.append(share(1, *held))
                held = None
        m = v * v
        C2[:, first:first + width] = m
        held = first, width, jnp.sum(m, axis=0, keepdims=True)
    shared.append(share(1, *held))

    for t, (lo, depth) in enumerate(PIECES_2):
        rescale(A2, C2, shared[t])
        d = dot(A2[:, lo:lo + depth], G[0, lo:lo + depth, :])
        if t == 0:
            C1[:, :COLS] = d
        elif t < len(PIECES_2) - 1:
            C1[:, :COLS] += d
        else:
            v = C1[:, :COLS] + d
            m = v * v
            last = share(2, 0, COLS, jnp.sum(m, axis=0, keepdims=True))
            for b in range(8):
                p = place(b)
                m_ref[:, 128 * b:128 * b + 128] = m[:, 128 * p:128 * p + 128]
    three(1, 0, ORDER, 0).wait_send()
    f = gathered(last)
    for b in range(8):
        p = place(b)
        r_ref[:, 128 * b:128 * b + 128] = f[:, 128 * p:128 * p + 128]
    three(2, 0, COLS, 0).wait_send()


def scale_kernel(m_ref, r_ref, out_hbm, out, sem):
    factor = r_ref[...]
    step = ROWS // 8
    for i in range(8):
        at = pl.ds(step * i, step)
        out[at, :] = m_ref[at, :] * factor
        pltpu.make_async_copy(out.at[at], out_hbm.at[at], sem).start()
    pltpu.make_async_copy(out, out_hbm, sem).wait()


def solution(mesh):
    block_spec = P(("graph", "row"), "col")

    def device_step(init_blk, graph_blk):
        dma = pltpu.SemaphoreType.DMA
        in_hbm = [pltpu.with_memory_space_constraint(v, pltpu.HBM) for v in (init_blk, graph_blk)]
        m, r = pl.pallas_call(
            mcl_kernel,
            name="mcl",
            out_shape=(jax.ShapeDtypeStruct((ROWS, COLS), F32), jax.ShapeDtypeStruct((1, COLS), F32)),
            in_specs=[pl.BlockSpec(memory_space=pltpu.HBM)] * 2,
            out_specs=(pl.BlockSpec(memory_space=pltpu.VMEM),) * 2,
            scratch_shapes=[
                pltpu.VMEM((ROWS, COLS), F32),
                pltpu.VMEM((ROWS, COLS), F32),
                pltpu.VMEM((2, ORDER, COLS), BF16),
                pltpu.VMEM((ROWS, ORDER), BF16),
                pltpu.VMEM((ROWS, ORDER), BF16),
                pltpu.VMEM((ROWS, ORDER), BF16),
                pltpu.VMEM((ROWS, ORDER), F32),
                pltpu.VMEM((ROWS, ORDER), F32),
                pltpu.VMEM((3, 4, 1, ORDER), F32),
                dma((3,)), dma((4,)),
                dma((NSUB,)), dma((NSUB,)), dma((NSUB + 1,)), dma((NKC,)),
                dma((NSUB,)), dma(()), dma((NSUB,)),
                dma((3,)), dma((len(PIECES_1) + len(PIECES_2) + 1,)),
            ],
            compiler_params=pltpu.CompilerParams(collective_id=0, has_side_effects=True, vmem_limit_bytes=48 * 2**20),
        )(*in_hbm)
        return pl.pallas_call(
            scale_kernel,
            name="scale",
            out_shape=jax.ShapeDtypeStruct((ROWS, COLS), F32),
            in_specs=[pl.BlockSpec(memory_space=pltpu.VMEM)] * 2,
            out_specs=pl.BlockSpec(memory_space=pltpu.HBM),
            scratch_shapes=[pltpu.VMEM((ROWS, COLS), F32), dma(())],
            compiler_params=pltpu.CompilerParams(vmem_limit_bytes=8 * 2**20),
        )(m, r)

    return jax.shard_map(device_step, mesh=mesh, in_specs=(block_spec, block_spec), out_specs=block_spec, check_vma=False)
```

```python
import jax
import jax.numpy as jnp
from jax import lax
from jax.experimental import pallas as pl
from jax.experimental.pallas import tpu as pltpu
from jax.sharding import PartitionSpec as P

MESH = pl.DeviceIdType.MESH
BF16 = jnp.bfloat16
F32 = jnp.float32

ROWS = 512
COLS = 1024
ORDER = 2048
SUB = 128
NSUB = ROWS // SUB
HALF = SUB // 2
LENT = 48
TAIL = (NSUB - 1, NSUB - 0.5)
KC = 256
NKC = COLS // KC
PIECES_1 = ((0, 512), (512, 512), (1024, 1024))
PIECES_2 = ((1024, 512), (1536, 512), (0, 512), (512, 512))


def place(b):
    return 2 * (b % 4) + b // 4


def mcl_kernel(a_hbm, g_hbm, m_ref, r_ref,
               a_f32, g_f32, G, A0, A1, A2, C1, C2, sums,
               ld_sem, snd, gx_r, gy_r, dx_r, ay_r, c0_r, c01_r, c2_r, c2x_r, c3_r, ar_s, ar_r):
    graph, col, row = lax.axis_index("graph"), lax.axis_index("col"), lax.axis_index("row")
    x, core = row // 2, row % 2
    nb_x = (graph, col, (1 - x) * 2 + core)
    nb_y = (graph, 1 - col, row)
    nb_c = (graph, col, x * 2 + 1 - core)
    nb_xc = (graph, col, (1 - x) * 2 + 1 - core)

    half_own = lax.rem(x + col, 2)
    half_far = 1 - half_own

    def position(half, side, sub):
        return pl.multiple_of(half * COLS + KC * (int(sub)) + SUB * side + int(SUB * (sub % 1)), HALF)

    def remote(ref_src, ref_dst, send, recv, dev):
        return pltpu.make_async_remote_copy(src_ref=ref_src, dst_ref=ref_dst, send_sem=send, recv_sem=recv,
                                            device_id=dev, device_id_type=MESH)

    loads = [pltpu.make_async_copy(src, dst, ld_sem.at[i]) for i, (src, dst) in enumerate((
        (g_hbm.at[pl.ds(0, SUB)], g_f32.at[pl.ds(0, SUB)]),
        (g_hbm.at[pl.ds(SUB, ROWS - SUB)], g_f32.at[pl.ds(SUB, ROWS - SUB)]),
        (a_hbm, a_f32)))]
    for cp in loads:
        cp.start()

    barrier = pltpu.get_barrier_semaphore()
    for dev in (nb_x, nb_y, nb_c, nb_xc):
        pl.semaphore_signal(barrier, inc=1, device_id=dev, device_id_type=MESH)

    def rows(hc, half, side, sub, n=SUB):
        return G.at[hc, pl.ds(position(half, side, sub), n)]

    own_at = [rows(0, half_own, core, i) for i in range(NSUB)]
    gx_at = [rows(0, half_far, core, i) for i in range(NSUB)]
    gy_at = [rows(1, half_own, core, i) for i in range(NSUB)]
    dx_at = [rows(1, half_far, core, i) for i in range(NSUB)]
    tail_y = [rows(1, half_own, core, i, HALF) for i in TAIL]
    tail_d = [rows(1, half_far, core, i, HALF) for i in TAIL]

    gx_cp = [remote(own_at[i], own_at[i], snd.at[0], gx_r.at[i], nb_x) for i in range(NSUB)]
    def last_rows(hc, half, extra):
        first = half * COLS + KC * (NSUB - 1)
        if extra:
            return G.at[hc, pl.ds(pl.multiple_of(first + 2 * (SUB - LENT), 16), 2 * LENT)]
        return G.at[hc, pl.ds(pl.multiple_of(first + (SUB - LENT) * core, 16), SUB - LENT)]

    gy_cp = [remote(own_at[i], dx_at[i], snd.at[0], gy_r.at[i], nb_y) for i in range(NSUB - 1)]
    gy_cp += [remote(last_rows(0, half_own, e), last_rows(1, half_far, e), snd.at[4 if e else 0], gy_r.at[NSUB - 1 + e], nb_y)
              for e in range(2)]
    dx_cp = [remote(at, at, snd.at[2], dx_r.at[i], nb_x) for i, at in enumerate(gy_at[:-1] + tail_y)]
    c0_cp = [remote(at, at, snd.at[0], c0_r if i == NSUB - 1 else c01_r.at[i], nb_c) for i, at in enumerate(own_at)]
    c1_cp = [remote(at, at, snd.at[1], c01_r.at[i], nb_c) for i, at in enumerate(gx_at)]
    c2_cp = [remote(at, at, snd.at[1], c2_r, nb_c) for at in gy_at[:-1]]
    c2_cp += [remote(last_rows(1, half_own, e), last_rows(1, half_own, e), snd.at[4 if e else 1], c2x_r if e else c2_r, nb_c)
              for e in range(2)]
    c3_cp = [remote(at, at, snd.at[3], c3_r.at[min(i, NSUB - 1)], nb_c) for i, at in enumerate(dx_at[:-1] + tail_d)]
    ay_cp = [remote(A0.at[:, pl.ds(KC * n, KC)], A0.at[:, pl.ds(COLS + KC * n, KC)], snd.at[2], ay_r.at[n], nb_y)
             for n in range(NKC)]

    def bytes_of(count, send, recv):
        at = G.at[0, pl.ds(0, count)] if count <= ORDER else G.at[:, pl.ds(0, count // 2)]
        return remote(at, at, send, recv, nb_c)

    def send_own(i):
        gx_cp[i].start()
        if i < NSUB - 1:
            gy_cp[i].start()
        c0_cp[i].start()

    for i in range(NSUB):
        if i < 2:
            loads[i].wait()
        for b in range(8):
            p = place(b)
            G[0, pl.ds(position(half_own, core, i), SUB), 128 * p:128 * p + 128] = (
                g_f32[SUB * i:SUB * (i + 1), 128 * b:128 * b + 128].astype(BF16))
        if i == 0:
            pl.semaphore_wait(barrier, 4)
        else:
            send_own(i - 1)
    loads[2].wait()
    for b in range(8):
        p = place(b)
        A0[:, 128 * p:128 * p + 128] = a_f32[:, 128 * b:128 * b + 128].astype(BF16)
    send_own(NSUB - 1)

    def dot(a, g):
        return jnp.dot(a, g, preferred_element_type=F32)

    def near_step(n):
        bytes_of((2 if n < NSUB - 1 else 1) * SUB, snd.at[0], c01_r.at[n]).wait_recv()
        d = dot(A0[:, KC * n:KC * n + KC], G[0, KC * n:KC * n + KC, :])
        if n == 0:
            C1[:, :COLS] = d
        else:
            C1[:, :COLS] += d

    for i in range(NSUB):
        gx_cp[i].wait_recv()
        c1_cp[i].start()
        gy_cp[i].wait_recv()
        c2_cp[i].start()
        if i == 0:
            c0_cp[-1].wait_recv()
            gy_cp[NSUB - 1].start()

            @pl.when(core == 1)
            def _():
                gy_cp[NSUB].start()

        if i == NSUB - 1:

            @pl.when(core == 1)
            def _():
                gy_cp[NSUB].wait_recv()
                c2_cp[NSUB].start()

        if i == NSUB - 2:
            dx_cp[0].start()
            ay_cp[0].start()
        if i >= 1:
            near_step(i - 1)
    dx_cp[1].start()
    ay_cp[1].start()
    near_step(NSUB - 1)
    bytes_of(ROWS - LENT, snd.at[1], c2_r).wait_recv()

    @pl.when(core == 0)
    def _():
        c2_cp[NSUB].wait_recv()

    slots = []

    def share(it, lo, width, value):
        index = len(slots)
        slots.append(index)
        sums[it, 0, :, lo:lo + width] = value
        for r, dev in ((1, nb_c), (2, nb_x), (3, nb_xc)):
            remote(sums.at[it, 0, :, pl.ds(lo, width)], sums.at[it, r, :, pl.ds(lo, width)],
                   ar_s.at[it], ar_r.at[index], dev).start()
        return it, lo, width, index

    def three(it, lo, width, index):
        at = sums.at[it, pl.ds(1, 3), :, pl.ds(lo, width)]
        return remote(at, at, ar_s.at[it], ar_r.at[index], nb_c)

    def gathered(handle):
        it, lo, width, index = handle
        three(it, lo, width, index).wait_recv()
        s = [sums[it, r, :, lo:lo + width] for r in range(4)]
        return float(ORDER) / ((s[0] + s[1]) + (s[2] + s[3]))

    def square_and_share(it, dst, lo, width, value):
        m = value * value
        dst[:, lo:lo + width] = m
        return share(it, lo, width, jnp.sum(m, axis=0, keepdims=True))

    def rescale(dst, src, handle):
        f = gathered(handle)
        lo, width = handle[1:3]
        dst[:, lo:lo + width] = (src[:, lo:lo + width] * f).astype(BF16)

    def graph(lo, depth, first, width):
        return G[first // COLS, lo:lo + depth, first % COLS:first % COLS + width]

    shared = []
    for n in range(NKC):
        if n == 0:
            bytes_of(3 * ROWS - LENT, snd.at[0], c2_r).wait_send()
        for i in (n,) if n < NSUB - 1 else (n, n + 1):
            dx_cp[i].wait_recv()
            c3_cp[i].start()
            if i + 2 < len(dx_cp):
                dx_cp[i + 2].start()
            if i == n == 2:
                bytes_of(2 * ROWS - LENT, snd.at[1], c2_r).wait_send()

                @pl.when(core == 1)
                def _():
                    bytes_of(4 * LENT, snd.at[4], c2_r).wait_send()

        ay_cp[n].wait_recv()
        if n + 2 < NKC:
            ay_cp[n + 2].start()
        lo = KC * n
        hi = COLS + lo
        if n < NKC - 1:
            C1[:, :COLS] += dot(A0[:, hi:hi + KC], G[0, hi:hi + KC, :])
        else:
            for first, width in PIECES_1:
                if first < COLS:
                    v = C1[:, first:first + width] + dot(A0[:, hi:hi + KC], graph(hi, KC, first, width))
                    shared.append(square_and_share(0, C1, first, width, v))
        bytes_of(SUB, snd.at[3], c3_r.at[n]).wait_recv()
        for first, width in PIECES_1:
            if first < COLS:
                continue
            d = dot(A0[:, lo:lo + KC], graph(lo, KC, first, width)) + dot(A0[:, hi:hi + KC], graph(hi, KC, first, width))
            if n == 0:
                C1[:, first:first + width] = d
            elif n < NKC - 1:
                C1[:, first:first + width] += d
            else:
                shared.append(square_and_share(0, C1, first, width, C1[:, first:first + width] + d))

    bytes_of(2 * ROWS, snd.at[2], c2_r).wait_send()
    bytes_of(ROWS, snd.at[3], c2_r).wait_send()
    done = 0
    for t in range(1):
        rescale(A1, C1, shared[t])
        lo, depth = PIECES_1[t]
        for hc in range(2):
            at = slice(hc * COLS, (hc + 1) * COLS)
            d = dot(A1[:, lo:lo + depth], G[hc, lo:lo + depth, :])
            if t == 0:
                C2[:, at] = d
            else:
                C2[:, at] += d
        done = lo + depth
    factors = [gathered(handle) for handle in shared[1:]]
    three(0, 0, ORDER, 0).wait_send()
    shared = []
    held = None
    for first, width in PIECES_2:
        v = C2[:, first:first + width]
        for (lo, depth), f in zip(PIECES_1[1:], factors):
            if first == PIECES_2[0][0]:
                A1[:, lo:lo + depth] = (C1[:, lo:lo + depth] * f).astype(BF16)
            v += dot(A1[:, lo:lo + depth], graph(lo, depth, first, width))
            if held is not None:
                shared.append(share(1, *held))
                held = None
        m = v * v
        C2[:, first:first + width] = m
        held = first, width, jnp.sum(m, axis=0, keepdims=True)
    shared.append(share(1, *held))

    for t, (lo, depth) in enumerate(PIECES_2):
        rescale(A2, C2, shared[t])
        d = dot(A2[:, lo:lo + depth], G[0, lo:lo + depth, :])
        if t == 0:
            C1[:, :COLS] = d
        elif t < len(PIECES_2) - 1:
            C1[:, :COLS] += d
        else:
            v = C1[:, :COLS] + d
            m = v * v
            last = share(2, 0, COLS, jnp.sum(m, axis=0, keepdims=True))
            for b in range(8):
                p = place(b)
                m_ref[:, 128 * b:128 * b + 128] = m[:, 128 * p:128 * p + 128]
    three(1, 0, ORDER, 0).wait_send()
    f = gathered(last)
    for b in range(8):
        p = place(b)
        r_ref[:, 128 * b:128 * b + 128] = f[:, 128 * p:128 * p + 128]
    three(2, 0, COLS, 0).wait_send()


def scale_kernel(m_ref, r_ref, out_hbm, out, sem):
    factor = r_ref[...]
    step = ROWS // 8
    for i in range(8):
        at = pl.ds(step * i, step)
        out[at, :] = m_ref[at, :] * factor
        pltpu.make_async_copy(out.at[at], out_hbm.at[at], sem).start()
    pltpu.make_async_copy(out, out_hbm, sem).wait()


def solution(mesh):
    block_spec = P(("graph", "row"), "col")

    def device_step(init_blk, graph_blk):
        dma = pltpu.SemaphoreType.DMA
        in_hbm = [pltpu.with_memory_space_constraint(v, pltpu.HBM) for v in (init_blk, graph_blk)]
        m, r = pl.pallas_call(
            mcl_kernel,
            name="mcl",
            out_shape=(jax.ShapeDtypeStruct((ROWS, COLS), F32), jax.ShapeDtypeStruct((1, COLS), F32)),
            in_specs=[pl.BlockSpec(memory_space=pltpu.HBM)] * 2,
            out_specs=(pl.BlockSpec(memory_space=pltpu.VMEM),) * 2,
            scratch_shapes=[
                pltpu.VMEM((ROWS, COLS), F32),
                pltpu.VMEM((ROWS, COLS), F32),
                pltpu.VMEM((2, ORDER, COLS), BF16),
                pltpu.VMEM((ROWS, ORDER), BF16),
                pltpu.VMEM((ROWS, ORDER), BF16),
                pltpu.VMEM((ROWS, ORDER), BF16),
                pltpu.VMEM((ROWS, ORDER), F32),
                pltpu.VMEM((ROWS, ORDER), F32),
                pltpu.VMEM((3, 4, 1, ORDER), F32),
                dma((3,)), dma((5,)),
                dma((NSUB,)), dma((NSUB + 1,)), dma((NSUB + 1,)), dma((NKC,)),
                dma(()), dma((NSUB,)), dma(()), dma(()), dma((NSUB,)),
                dma((3,)), dma((len(PIECES_1) + len(PIECES_2) + 1,)),
            ],
            compiler_params=pltpu.CompilerParams(collective_id=0, has_side_effects=True, vmem_limit_bytes=48 * 2**20),
        )(*in_hbm)
        return pl.pallas_call(
            scale_kernel,
            name="scale",
            out_shape=jax.ShapeDtypeStruct((ROWS, COLS), F32),
            in_specs=[pl.BlockSpec(memory_space=pltpu.VMEM)] * 2,
            out_specs=pl.BlockSpec(memory_space=pltpu.HBM),
            scratch_shapes=[pltpu.VMEM((ROWS, COLS), F32), dma(())],
            compiler_params=pltpu.CompilerParams(vmem_limit_bytes=8 * 2**20),
        )(m, r)

    return jax.shard_map(device_step, mesh=mesh, in_specs=(block_spec, block_spec), out_specs=block_spec, check_vma=False)
```

```python
import jax
import jax.numpy as jnp
from jax import lax
from jax.experimental import pallas as pl
from jax.experimental.pallas import tpu as pltpu
from jax.sharding import PartitionSpec as P

MESH = pl.DeviceIdType.MESH
BF16 = jnp.bfloat16
F32 = jnp.float32

ROWS = 512
COLS = 1024
ORDER = 2048
SUB = 128
NSUB = ROWS // SUB
HALF = SUB // 2
LENT = 48
TAIL = (NSUB - 1, NSUB - 0.5)
KC = 256
NKC = COLS // KC
PIECES_1 = ((0, 512), (512, 512), (1024, 1024))
EARLY = 2
STEP = 512
PIECES_2 = ((1024, 512), (1536, 512), (0, 512), (512, 512))


def place(b):
    return 2 * (b % 4) + b // 4


def mcl_kernel(a_hbm, g_hbm, m_ref, r_ref,
               a_f32, g_f32, G, A0, A1, A2, C1, C2, sums,
               ld_sem, snd, in_r, far_r, c0_r, c01_r, c2_r, c2x_r, c3_r, ar_s, ar_r):
    graph, col, row = lax.axis_index("graph"), lax.axis_index("col"), lax.axis_index("row")
    x, core = row // 2, row % 2
    nb_x = (graph, col, (1 - x) * 2 + core)
    nb_y = (graph, 1 - col, row)
    nb_c = (graph, col, x * 2 + 1 - core)
    nb_xc = (graph, col, (1 - x) * 2 + 1 - core)

    half_own = lax.rem(x + col, 2)
    half_far = 1 - half_own

    def position(half, side, sub):
        return pl.multiple_of(half * COLS + KC * (int(sub)) + SUB * side + int(SUB * (sub % 1)), HALF)

    def remote(ref_src, ref_dst, send, recv, dev):
        return pltpu.make_async_remote_copy(src_ref=ref_src, dst_ref=ref_dst, send_sem=send, recv_sem=recv,
                                            device_id=dev, device_id_type=MESH)

    loads = [pltpu.make_async_copy(src, dst, ld_sem.at[i]) for i, (src, dst) in enumerate((
        (g_hbm.at[pl.ds(0, SUB)], g_f32.at[pl.ds(0, SUB)]),
        (g_hbm.at[pl.ds(SUB, ROWS - SUB)], g_f32.at[pl.ds(SUB, ROWS - SUB)]),
        (a_hbm, a_f32)))]
    for cp in loads:
        cp.start()

    barrier = pltpu.get_barrier_semaphore()
    for dev in (nb_x, nb_y, nb_c, nb_xc):
        pl.semaphore_signal(barrier, inc=1, device_id=dev, device_id_type=MESH)

    def rows(hc, half, side, sub, n=SUB):
        return G.at[hc, pl.ds(position(half, side, sub), n)]

    own_at = [rows(0, half_own, core, i) for i in range(NSUB)]
    gx_at = [rows(0, half_far, core, i) for i in range(NSUB)]
    gy_at = [rows(1, half_own, core, i) for i in range(NSUB)]
    dx_at = [rows(1, half_far, core, i) for i in range(NSUB)]
    tail_y = [rows(1, half_own, core, i, HALF) for i in TAIL]
    tail_d = [rows(1, half_far, core, i, HALF) for i in TAIL]

    gx_cp = [remote(own_at[i], own_at[i], snd.at[0], in_r.at[i // 2], nb_x) for i in range(NSUB)]
    def last_rows(hc, half, extra):
        first = half * COLS + KC * (NSUB - 1)
        if extra:
            return G.at[hc, pl.ds(pl.multiple_of(first + 2 * (SUB - LENT), 16), 2 * LENT)]
        return G.at[hc, pl.ds(pl.multiple_of(first + (SUB - LENT) * core, 16), SUB - LENT)]

    gy_cp = [remote(own_at[i], dx_at[i], snd.at[0], in_r.at[i // 2], nb_y) for i in range(NSUB - 1)]
    gy_cp += [remote(last_rows(0, half_own, e), last_rows(1, half_far, e), snd.at[3 if e else 0], in_r.at[1 + e], nb_y)
              for e in range(2)]
    dx_cp = [remote(at, at, snd.at[2], far_r.at[i], nb_x) for i, at in enumerate(gy_at[:-1] + tail_y)]
    c0_cp = [remote(at, at, snd.at[0], c0_r if i == NSUB - 1 else c01_r, nb_c) for i, at in enumerate(own_at)]
    c1_cp = [remote(at, at, snd.at[1], c01_r, nb_c) for at in gx_at]
    c2_cp = [remote(at, at, snd.at[1], c2_r, nb_c) for at in gy_at[:-1]]
    c2_cp += [remote(last_rows(1, half_own, e), last_rows(1, half_own, e), snd.at[3 if e else 1], c2x_r if e else c2_r, nb_c)
              for e in range(2)]
    c3_cp = [remote(at, at, snd.at[0], c3_r.at[min(i, NSUB - 1)], nb_c) for i, at in enumerate(dx_at[:-1] + tail_d)]
    ay_cp = [remote(A0.at[:, pl.ds(KC * n, KC)], A0.at[:, pl.ds(COLS + KC * n, KC)], snd.at[2], far_r.at[n if n < NKC - 1 else NSUB + 1], nb_y)
             for n in range(NKC)]

    def bytes_of(count, send, recv):
        at = G.at[0, pl.ds(0, count)] if count <= ORDER else G.at[:, pl.ds(0, count // 2)]
        return remote(at, at, send, recv, nb_c)

    def send_own(i):
        gx_cp[i].start()
        if i < NSUB - 1:
            gy_cp[i].start()
        c0_cp[i].start()

    for i in range(NSUB):
        if i < 2:
            loads[i].wait()
        for b in range(8):
            p = place(b)
            G[0, pl.ds(position(half_own, core, i), SUB), 128 * p:128 * p + 128] = (
                g_f32[SUB * i:SUB * (i + 1), 128 * b:128 * b + 128].astype(BF16))
        if i == 0:
            pl.semaphore_wait(barrier, 4)
        else:
            send_own(i - 1)
    loads[2].wait()
    for b in range(8):
        p = place(b)
        A0[:, 128 * p:128 * p + 128] = a_f32[:, 128 * b:128 * b + 128].astype(BF16)
    send_own(NSUB - 1)

    def dot(a, g):
        return jnp.dot(a, g, preferred_element_type=F32)

    c0_cp[-1].wait_recv()
    gy_cp[NSUB - 1].start()

    @pl.when(core == 1)
    def _():
        gy_cp[NSUB].start()

    for half in range(2):
        bytes_of(4 * SUB - half * LENT, snd.at[0], in_r.at[half]).wait_recv()
        for i in (2 * half, 2 * half + 1):
            c1_cp[i].start()
            c2_cp[i].start()
        if half == 0:
            for i in range(2):
                dx_cp[i].start()
                ay_cp[i].start()

    @pl.when(core == 1)
    def _():
        gy_cp[NSUB].wait_recv()
        c2_cp[NSUB].start()

    bytes_of(7 * SUB, snd.at[0], c01_r).wait_recv()
    C1[:, :COLS] = dot(A0[:, :COLS], G[0, :COLS, :])
    bytes_of(ROWS - LENT, snd.at[1], c2_r).wait_recv()

    @pl.when(core == 0)
    def _():
        c2_cp[NSUB].wait_recv()

    slots = []

    def share(it, lo, width, value):
        index = len(slots)
        slots.append(index)
        sums[it, 0, :, lo:lo + width] = value
        for r, dev in ((1, nb_c), (2, nb_x), (3, nb_xc)):
            remote(sums.at[it, 0, :, pl.ds(lo, width)], sums.at[it, r, :, pl.ds(lo, width)],
                   ar_s, ar_r.at[index], dev).start()
        return it, lo, width, index

    def three(it, lo, width, index):
        at = sums.at[it, pl.ds(1, 3), :, pl.ds(lo, width)]
        return remote(at, at, ar_s, ar_r.at[index], nb_c)

    def gathered(handle):
        it, lo, width, index = handle
        three(it, lo, width, index).wait_recv()
        s = [sums[it, r, :, lo:lo + width] for r in range(4)]
        return float(ORDER) / ((s[0] + s[1]) + (s[2] + s[3]))

    def square_and_share(it, dst, lo, width, value):
        m = value * value
        dst[:, lo:lo + width] = m
        return share(it, lo, width, jnp.sum(m, axis=0, keepdims=True))

    def rescale(dst, src, handle):
        f = gathered(handle)
        lo, width = handle[1:3]
        dst[:, lo:lo + width] = (src[:, lo:lo + width] * f).astype(BF16)

    def graph(lo, depth, first, width):
        return G[first // COLS, lo:lo + depth, first % COLS:first % COLS + width]

    def far_piece(i):
        dx_cp[i].wait_recv()
        c3_cp[i].start()

    bytes_of(3 * ROWS - LENT, snd.at[0], c2_r).wait_send()
    shared = []
    for n in range(NKC):
        if n < NKC - 1:
            bytes_of(2 * SUB, snd.at[0], far_r.at[n]).wait_recv()
            c3_cp[n].start()
        else:
            far_piece(n)
        for i in ((2,), (3, 4), (), ())[n]:
            dx_cp[i].start()
        if n + 2 < NKC:
            ay_cp[n + 2].start()
        if n == 2:
            bytes_of(2 * ROWS - LENT, snd.at[1], c2_r).wait_send()

            @pl.when(core == 1)
            def _():
                bytes_of(4 * LENT, snd.at[3], c2_r).wait_send()

        if n == NKC - 1:

            @pl.when(core == 1)
            def _():
                far_piece(NSUB)

            ay_cp[n].wait_recv()
        lo = KC * n
        hi = COLS + lo
        if n < NKC - 1:
            C1[:, :COLS] += dot(A0[:, hi:hi + KC], G[0, hi:hi + KC, :])
        else:
            for first, width in PIECES_1:
                if first < COLS:
                    v = C1[:, first:first + width] + dot(A0[:, hi:hi + KC], graph(hi, KC, first, width))
                    shared.append(square_and_share(0, C1, first, width, v))
                    if len(shared) == 1:

                        @pl.when(core == 0)
                        def _():
                            far_piece(NSUB)

        bytes_of(SUB, snd.at[0], c3_r.at[n]).wait_recv()
        for first, width in PIECES_1:
            if first < COLS:
                continue
            d = dot(A0[:, lo:lo + KC], graph(lo, KC, first, width)) + dot(A0[:, hi:hi + KC], graph(hi, KC, first, width))
            if n == 0:
                C1[:, first:first + width] = d
            elif n < NKC - 1:
                C1[:, first:first + width] += d
            else:
                shared.append(square_and_share(0, C1, first, width, C1[:, first:first + width] + d))

    bytes_of(2 * ROWS, snd.at[2], c2_r).wait_send()
    bytes_of(ROWS, snd.at[0], c2_r).wait_send()
    done = 0
    for t in range(1):
        rescale(A1, C1, shared[t])
        lo, depth = PIECES_1[t]
        for hc in range(2):
            at = slice(hc * COLS, (hc + 1) * COLS)
            d = dot(A1[:, lo:lo + depth], G[hc, lo:lo + depth, :])
            if t == 0:
                C2[:, at] = d
            else:
                C2[:, at] += d
        done = lo + depth
    rescale(A1, C1, shared[1])
    lo, depth = PIECES_1[1]
    for first, width in PIECES_2[:EARLY]:
        C2[:, first:first + width] += dot(A1[:, lo:lo + depth], graph(lo, depth, first, width))
    f = gathered(shared[2])
    three(0, 0, ORDER, 0).wait_send()
    shared = []
    held = None
    for t, (first, width) in enumerate(PIECES_2):
        v = C2[:, first:first + width]
        for lo, depth in PIECES_1[2 if t < EARLY else 1:]:
            for at in range(lo, lo + depth, STEP):
                if t == 0:
                    A1[:, at:at + STEP] = (C1[:, at:at + STEP] * f[:, at - lo:at - lo + STEP]).astype(BF16)
                v += dot(A1[:, at:at + STEP], graph(at, STEP, first, width))
                if held is not None:
                    shared.append(share(1, *held))
                    held = None
        m = v * v
        C2[:, first:first + width] = m
        held = first, width, jnp.sum(m, axis=0, keepdims=True)
    shared.append(share(1, *held))

    for t, (lo, depth) in enumerate(PIECES_2):
        rescale(A2, C2, shared[t])
        if t == len(PIECES_2) - 1:
            three(1, 0, ORDER, 0).wait_send()
        d = dot(A2[:, lo:lo + depth], G[0, lo:lo + depth, :])
        if t == 0:
            C1[:, :COLS] = d
        elif t < len(PIECES_2) - 1:
            C1[:, :COLS] += d
        else:
            v = C1[:, :COLS] + d
            m = v * v
            last = share(2, 0, COLS, jnp.sum(m, axis=0, keepdims=True))
            for b in range(8):
                p = place(b)
                m_ref[:, 128 * b:128 * b + 128] = m[:, 128 * p:128 * p + 128]
    f = gathered(last)
    for b in range(8):
        p = place(b)
        r_ref[:, 128 * b:128 * b + 128] = f[:, 128 * p:128 * p + 128]
    three(2, 0, COLS, 0).wait_send()


def scale_kernel(m_ref, r_ref, out_hbm, out, sem):
    factor = r_ref[...]
    step = ROWS // 8
    for i in range(8):
        at = pl.ds(step * i, step)
        out[at, :] = m_ref[at, :] * factor
        pltpu.make_async_copy(out.at[at], out_hbm.at[at], sem).start()
    pltpu.make_async_copy(out, out_hbm, sem).wait()


def solution(mesh):
    block_spec = P(("graph", "row"), "col")

    def device_step(init_blk, graph_blk):
        dma = pltpu.SemaphoreType.DMA
        in_hbm = [pltpu.with_memory_space_constraint(v, pltpu.HBM) for v in (init_blk, graph_blk)]
        m, r = pl.pallas_call(
            mcl_kernel,
            name="mcl",
            out_shape=(jax.ShapeDtypeStruct((ROWS, COLS), F32), jax.ShapeDtypeStruct((1, COLS), F32)),
            in_specs=[pl.BlockSpec(memory_space=pltpu.HBM)] * 2,
            out_specs=(pl.BlockSpec(memory_space=pltpu.VMEM),) * 2,
            scratch_shapes=[
                pltpu.VMEM((ROWS, COLS), F32),
                pltpu.VMEM((ROWS, COLS), F32),
                pltpu.VMEM((2, ORDER, COLS), BF16),
                pltpu.VMEM((ROWS, ORDER), BF16),
                pltpu.VMEM((ROWS, ORDER), BF16),
                pltpu.VMEM((ROWS, ORDER), BF16),
                pltpu.VMEM((ROWS, ORDER), F32),
                pltpu.VMEM((ROWS, ORDER), F32),
                pltpu.VMEM((3, 4, 1, ORDER), F32),
                dma((3,)), dma((4,)), dma((3,)), dma((NSUB + 2,)),
                dma(()), dma(()), dma(()), dma(()), dma((NSUB,)),
                dma(()), dma((len(PIECES_1) + len(PIECES_2) + 1,)),
            ],
            compiler_params=pltpu.CompilerParams(collective_id=0, has_side_effects=True, vmem_limit_bytes=48 * 2**20),
        )(*in_hbm)
        return pl.pallas_call(
            scale_kernel,
            name="scale",
            out_shape=jax.ShapeDtypeStruct((ROWS, COLS), F32),
            in_specs=[pl.BlockSpec(memory_space=pltpu.VMEM)] * 2,
            out_specs=pl.BlockSpec(memory_space=pltpu.HBM),
            scratch_shapes=[pltpu.VMEM((ROWS, COLS), F32), dma(())],
            compiler_params=pltpu.CompilerParams(vmem_limit_bytes=8 * 2**20),
        )(m, r)

    return jax.shard_map(device_step, mesh=mesh, in_specs=(block_spec, block_spec), out_specs=block_spec, check_vma=False)
```

```python
import jax
import jax.numpy as jnp
from jax import lax
from jax.experimental import pallas as pl
from jax.experimental.pallas import tpu as pltpu
from jax.sharding import PartitionSpec as P

MESH = pl.DeviceIdType.MESH
BF16 = jnp.bfloat16
F32 = jnp.float32

ROWS = 512
COLS = 1024
ORDER = 2048
SUB = 128
NSUB = ROWS // SUB
HALF = SUB // 2
FIRST = 32
LENT = 48
TAIL = (NSUB - 1, NSUB - 0.5)
KC = 256
NKC = COLS // KC
PIECES_1 = ((0, 512), (512, 512), (1024, 1024))
EARLY = 2
STEP = 512
PIECES_2 = ((1024, 512), (1536, 512), (0, 512), (512, 512))


def place(b):
    return 2 * (b % 4) + b // 4


def mcl_kernel(a_hbm, g_hbm, m_ref, r_ref,
               a_f32, g_f32, G, A0, A1, A2, C1, C2, sums,
               ld_sem, snd, in_r, far_r, c0_r, c01_r, c2_r, c2x_r, c3_r, ar_s, ar_r):
    graph, col, row = lax.axis_index("graph"), lax.axis_index("col"), lax.axis_index("row")
    x, core = row // 2, row % 2
    nb_x = (graph, col, (1 - x) * 2 + core)
    nb_y = (graph, 1 - col, row)
    nb_c = (graph, col, x * 2 + 1 - core)
    nb_xc = (graph, col, (1 - x) * 2 + 1 - core)

    half_own = lax.rem(x + col, 2)
    half_far = 1 - half_own

    def position(half, side, sub):
        return pl.multiple_of(half * COLS + KC * (int(sub)) + SUB * side + int(SUB * (sub % 1)), HALF)

    def remote(ref_src, ref_dst, send, recv, dev):
        return pltpu.make_async_remote_copy(src_ref=ref_src, dst_ref=ref_dst, send_sem=send, recv_sem=recv,
                                            device_id=dev, device_id_type=MESH)

    cuts = (0, FIRST, 2 * FIRST, SUB, 2 * SUB, ROWS)
    loads = [pltpu.make_async_copy(g_hbm.at[pl.ds(lo, hi - lo)], g_f32.at[pl.ds(lo, hi - lo)], ld_sem.at[i])
             for i, (lo, hi) in enumerate(zip(cuts, cuts[1:]))]
    loads.append(pltpu.make_async_copy(a_hbm, a_f32, ld_sem.at[len(loads)]))
    for cp in loads:
        cp.start()

    barrier = pltpu.get_barrier_semaphore()
    for dev in (nb_x, nb_y, nb_c, nb_xc):
        pl.semaphore_signal(barrier, inc=1, device_id=dev, device_id_type=MESH)

    def rows(hc, half, side, sub, n=SUB):
        return G.at[hc, pl.ds(position(half, side, sub), n)]

    own_at = [rows(0, half_own, core, i) for i in range(NSUB)]
    gx_at = [rows(0, half_far, core, i) for i in range(NSUB)]
    gy_at = [rows(1, half_own, core, i) for i in range(NSUB)]
    dx_at = [rows(1, half_far, core, i) for i in range(NSUB)]
    tail_y = [rows(1, half_own, core, i, HALF) for i in TAIL]
    tail_d = [rows(1, half_far, core, i, HALF) for i in TAIL]

    gx_cp = [remote(own_at[i], own_at[i], snd.at[0], in_r.at[i // 2], nb_x) for i in range(NSUB)]
    def last_rows(hc, half, extra):
        first = half * COLS + KC * (NSUB - 1)
        if extra:
            return G.at[hc, pl.ds(pl.multiple_of(first + 2 * (SUB - LENT), 16), 2 * LENT)]
        return G.at[hc, pl.ds(pl.multiple_of(first + (SUB - LENT) * core, 16), SUB - LENT)]

    gy_cp = [remote(own_at[i], dx_at[i], snd.at[0], in_r.at[i // 2], nb_y) for i in range(NSUB - 1)]
    gy_cp += [remote(last_rows(0, half_own, e), last_rows(1, half_far, e), snd.at[3 if e else 0], in_r.at[1 + e], nb_y)
              for e in range(2)]
    dx_cp = [remote(at, at, snd.at[2], far_r.at[i], nb_x) for i, at in enumerate(gy_at[:-1] + tail_y)]
    c0_cp = [remote(at, at, snd.at[0], c0_r if i == NSUB - 1 else c01_r, nb_c) for i, at in enumerate(own_at)]
    c1_cp = [remote(at, at, snd.at[1], c01_r, nb_c) for at in gx_at]
    c2_cp = [remote(at, at, snd.at[1], c2_r, nb_c) for at in gy_at[:-1]]
    c2_cp += [remote(last_rows(1, half_own, e), last_rows(1, half_own, e), snd.at[3 if e else 1], c2x_r if e else c2_r, nb_c)
              for e in range(2)]
    c3_cp = [remote(at, at, snd.at[0], c3_r.at[min(i, NSUB - 1)], nb_c) for i, at in enumerate(dx_at[:-1] + tail_d)]
    ay_cp = [remote(A0.at[:, pl.ds(KC * n, KC)], A0.at[:, pl.ds(COLS + KC * n, KC)], snd.at[2], far_r.at[n if n < NKC - 1 else NSUB + 1], nb_y)
             for n in range(NKC)]

    def bytes_of(count, send, recv):
        at = G.at[0, pl.ds(0, count)] if count <= ORDER else G.at[:, pl.ds(0, count // 2)]
        return remote(at, at, send, recv, nb_c)

    def send_own(lo, hi):
        i = lo // SUB
        if hi - lo == SUB:
            gx_cp[i].start()
            if i < NSUB - 1:
                gy_cp[i].start()
            c0_cp[i].start()
        else:
            at = G.at[0, pl.ds(pl.multiple_of(position(half_own, core, 0) + lo, FIRST), hi - lo)]
            there = G.at[1, pl.ds(pl.multiple_of(position(half_far, core, 0) + lo, FIRST), hi - lo)]
            remote(at, at, snd.at[0], in_r.at[0], nb_x).start()
            remote(at, there, snd.at[0], in_r.at[0], nb_y).start()
            remote(at, at, snd.at[0], c01_r, nb_c).start()

    parts = (*zip(cuts, cuts[1:4]), *((SUB * i, SUB * (i + 1)) for i in range(1, NSUB)))
    for t, (lo, hi) in enumerate(parts):
        if lo in cuts:
            loads[cuts.index(lo)].wait()
        for b in range(8):
            p = place(b)
            G[0, pl.ds(pl.multiple_of(position(half_own, core, lo // SUB) + lo % SUB, FIRST), hi - lo), 128 * p:128 * p + 128] = (
                g_f32[lo:hi, 128 * b:128 * b + 128].astype(BF16))
        if t == 0:
            pl.semaphore_wait(barrier, 4)
        else:
            send_own(*parts[t - 1])
    loads[-1].wait()
    for b in range(8):
        p = place(b)
        A0[:, 128 * p:128 * p + 128] = a_f32[:, 128 * b:128 * b + 128].astype(BF16)
    send_own(*parts[-1])

    def dot(a, g):
        return jnp.dot(a, g, preferred_element_type=F32)

    c0_cp[-1].wait_recv()
    gy_cp[NSUB - 1].start()

    @pl.when(core == 1)
    def _():
        gy_cp[NSUB].start()

    for half in range(2):
        bytes_of(4 * SUB - half * LENT, snd.at[0], in_r.at[half]).wait_recv()
        for i in (2 * half, 2 * half + 1):
            c1_cp[i].start()
            c2_cp[i].start()
        if half == 0:
            for i in range(2):
                dx_cp[i].start()
                ay_cp[i].start()

    @pl.when(core == 1)
    def _():
        gy_cp[NSUB].wait_recv()
        c2_cp[NSUB].start()

    bytes_of(7 * SUB, snd.at[0], c01_r).wait_recv()
    C1[:, :COLS] = dot(A0[:, :COLS], G[0, :COLS, :])
    bytes_of(ROWS - LENT, snd.at[1], c2_r).wait_recv()

    @pl.when(core == 0)
    def _():
        c2_cp[NSUB].wait_recv()

    slots = []

    def share(it, lo, width, value):
        index = len(slots)
        slots.append(index)
        sums[it, 0, :, lo:lo + width] = value
        for r, dev in ((1, nb_c), (2, nb_x), (3, nb_xc)):
            remote(sums.at[it, 0, :, pl.ds(lo, width)], sums.at[it, r, :, pl.ds(lo, width)],
                   ar_s, ar_r.at[index], dev).start()
        return it, lo, width, index

    def three(it, lo, width, index):
        at = sums.at[it, pl.ds(1, 3), :, pl.ds(lo, width)]
        return remote(at, at, ar_s, ar_r.at[index], nb_c)

    def gathered(handle):
        it, lo, width, index = handle
        three(it, lo, width, index).wait_recv()
        s = [sums[it, r, :, lo:lo + width] for r in range(4)]
        return float(ORDER) / ((s[0] + s[1]) + (s[2] + s[3]))

    def square_and_share(it, dst, lo, width, value):
        m = value * value
        dst[:, lo:lo + width] = m
        return share(it, lo, width, jnp.sum(m, axis=0, keepdims=True))

    def rescale(dst, src, handle):
        f = gathered(handle)
        lo, width = handle[1:3]
        dst[:, lo:lo + width] = (src[:, lo:lo + width] * f).astype(BF16)

    def graph(lo, depth, first, width):
        return G[first // COLS, lo:lo + depth, first % COLS:first % COLS + width]

    def far_piece(i):
        dx_cp[i].wait_recv()
        c3_cp[i].start()

    bytes_of(3 * ROWS - LENT, snd.at[0], c2_r).wait_send()
    shared = []
    for n in range(NKC):
        if n < NKC - 1:
            bytes_of(2 * SUB, snd.at[0], far_r.at[n]).wait_recv()
            c3_cp[n].start()
        else:
            far_piece(n)
        for i in ((2,), (3, 4), (), ())[n]:
            dx_cp[i].start()
        if n + 2 < NKC:
            ay_cp[n + 2].start()
        if n == 2:
            bytes_of(2 * ROWS - LENT, snd.at[1], c2_r).wait_send()

            @pl.when(core == 1)
            def _():
                bytes_of(4 * LENT, snd.at[3], c2_r).wait_send()

        if n == NKC - 1:

            @pl.when(core == 1)
            def _():
                far_piece(NSUB)

            ay_cp[n].wait_recv()
        lo = KC * n
        hi = COLS + lo
        if n < NKC - 1:
            C1[:, :COLS] += dot(A0[:, hi:hi + KC], G[0, hi:hi + KC, :])
        else:
            for first, width in PIECES_1:
                if first < COLS:
                    v = C1[:, first:first + width] + dot(A0[:, hi:hi + KC], graph(hi, KC, first, width))
                    shared.append(square_and_share(0, C1, first, width, v))
                    if len(shared) == 1:

                        @pl.when(core == 0)
                        def _():
                            far_piece(NSUB)

        bytes_of(SUB, snd.at[0], c3_r.at[n]).wait_recv()
        for first, width in PIECES_1:
            if first < COLS:
                continue
            d = dot(A0[:, lo:lo + KC], graph(lo, KC, first, width)) + dot(A0[:, hi:hi + KC], graph(hi, KC, first, width))
            if n == 0:
                C1[:, first:first + width] = d
            elif n < NKC - 1:
                C1[:, first:first + width] += d
            else:
                shared.append(square_and_share(0, C1, first, width, C1[:, first:first + width] + d))

    bytes_of(2 * ROWS, snd.at[2], c2_r).wait_send()
    bytes_of(ROWS, snd.at[0], c2_r).wait_send()
    done = 0
    for t in range(1):
        rescale(A1, C1, shared[t])
        lo, depth = PIECES_1[t]
        for hc in range(2):
            at = slice(hc * COLS, (hc + 1) * COLS)
            d = dot(A1[:, lo:lo + depth], G[hc, lo:lo + depth, :])
            if t == 0:
                C2[:, at] = d
            else:
                C2[:, at] += d
        done = lo + depth
    rescale(A1, C1, shared[1])
    lo, depth = PIECES_1[1]
    for first, width in PIECES_2[:EARLY]:
        C2[:, first:first + width] += dot(A1[:, lo:lo + depth], graph(lo, depth, first, width))
    f = gathered(shared[2])
    three(0, 0, ORDER, 0).wait_send()
    shared = []
    held = None
    for t, (first, width) in enumerate(PIECES_2):
        v = C2[:, first:first + width]
        for lo, depth in PIECES_1[2 if t < EARLY else 1:]:
            for at in range(lo, lo + depth, STEP):
                if t == 0:
                    A1[:, at:at + STEP] = (C1[:, at:at + STEP] * f[:, at - lo:at - lo + STEP]).astype(BF16)
                v += dot(A1[:, at:at + STEP], graph(at, STEP, first, width))
                if held is not None:
                    shared.append(share(1, *held))
                    held = None
        m = v * v
        C2[:, first:first + width] = m
        held = first, width, jnp.sum(m, axis=0, keepdims=True)
    shared.append(share(1, *held))

    for t, (lo, depth) in enumerate(PIECES_2):
        rescale(A2, C2, shared[t])
        if t == len(PIECES_2) - 1:
            three(1, 0, ORDER, 0).wait_send()
        d = dot(A2[:, lo:lo + depth], G[0, lo:lo + depth, :])
        if t == 0:
            C1[:, :COLS] = d
        elif t < len(PIECES_2) - 1:
            C1[:, :COLS] += d
        else:
            v = C1[:, :COLS] + d
            m = v * v
            last = share(2, 0, COLS, jnp.sum(m, axis=0, keepdims=True))
            for b in range(8):
                p = place(b)
                m_ref[:, 128 * b:128 * b + 128] = m[:, 128 * p:128 * p + 128]
    f = gathered(last)
    for b in range(8):
        p = place(b)
        r_ref[:, 128 * b:128 * b + 128] = f[:, 128 * p:128 * p + 128]
    three(2, 0, COLS, 0).wait_send()


def scale_kernel(m_ref, r_ref, out_hbm, out, sem):
    factor = r_ref[...]
    step = ROWS // 8
    for i in range(8):
        at = pl.ds(step * i, step)
        out[at, :] = m_ref[at, :] * factor
        pltpu.make_async_copy(out.at[at], out_hbm.at[at], sem).start()
    pltpu.make_async_copy(out, out_hbm, sem).wait()


def solution(mesh):
    block_spec = P(("graph", "row"), "col")

    def device_step(init_blk, graph_blk):
        dma = pltpu.SemaphoreType.DMA
        in_hbm = [pltpu.with_memory_space_constraint(v, pltpu.HBM) for v in (init_blk, graph_blk)]
        m, r = pl.pallas_call(
            mcl_kernel,
            name="mcl",
            out_shape=(jax.ShapeDtypeStruct((ROWS, COLS), F32), jax.ShapeDtypeStruct((1, COLS), F32)),
            in_specs=[pl.BlockSpec(memory_space=pltpu.HBM)] * 2,
            out_specs=(pl.BlockSpec(memory_space=pltpu.VMEM),) * 2,
            scratch_shapes=[
                pltpu.VMEM((ROWS, COLS), F32),
                pltpu.VMEM((ROWS, COLS), F32),
                pltpu.VMEM((2, ORDER, COLS), BF16),
                pltpu.VMEM((ROWS, ORDER), BF16),
                pltpu.VMEM((ROWS, ORDER), BF16),
                pltpu.VMEM((ROWS, ORDER), BF16),
                pltpu.VMEM((ROWS, ORDER), F32),
                pltpu.VMEM((ROWS, ORDER), F32),
                pltpu.VMEM((3, 4, 1, ORDER), F32),
                dma((6,)), dma((4,)), dma((3,)), dma((NSUB + 2,)),
                dma(()), dma(()), dma(()), dma(()), dma((NSUB,)),
                dma(()), dma((len(PIECES_1) + len(PIECES_2) + 1,)),
            ],
            compiler_params=pltpu.CompilerParams(collective_id=0, has_side_effects=True, vmem_limit_bytes=48 * 2**20),
        )(*in_hbm)
        return pl.pallas_call(
            scale_kernel,
            name="scale",
            out_shape=jax.ShapeDtypeStruct((ROWS, COLS), F32),
            in_specs=[pl.BlockSpec(memory_space=pltpu.VMEM)] * 2,
            out_specs=pl.BlockSpec(memory_space=pltpu.HBM),
            scratch_shapes=[pltpu.VMEM((ROWS, COLS), F32), dma(())],
            compiler_params=pltpu.CompilerParams(vmem_limit_bytes=8 * 2**20),
        )(m, r)

    return jax.shard_map(device_step, mesh=mesh, in_specs=(block_spec, block_spec), out_specs=block_spec, check_vma=False)
```

```python
import jax
import jax.numpy as jnp
from jax import lax
from jax.experimental import pallas as pl
from jax.experimental.pallas import tpu as pltpu
from jax.sharding import PartitionSpec as P

MESH = pl.DeviceIdType.MESH
BF16 = jnp.bfloat16
F32 = jnp.float32

ROWS = 512
COLS = 1024
ORDER = 2048
SUB = 128
NSUB = ROWS // SUB
HALF = SUB // 2
FIRST = 32
LENT = 48
TAIL = (NSUB - 1, NSUB - 0.5)
KC = 256
NKC = COLS // KC
PIECES_1 = ((0, 512), (512, 512), (1024, 1024))
EARLY = 2
STEP = 512
PIECES_2 = ((1024, 512), (1536, 512), (0, 512), (512, 512))


def place(b):
    return 2 * (b % 4) + b // 4


def mcl_kernel(a_hbm, g_hbm, m_ref, r_ref,
               a_f32, g_f32, G, A0, A1, A2, C1, C2, sums,
               ld_sem, snd, in_r, far_r, c0_r, c01_r, c2_r, c2x_r, c3_r, ar_s, ar_r):
    graph, col, row = lax.axis_index("graph"), lax.axis_index("col"), lax.axis_index("row")
    x, core = row // 2, row % 2
    nb_x = (graph, col, (1 - x) * 2 + core)
    nb_y = (graph, 1 - col, row)
    nb_c = (graph, col, x * 2 + 1 - core)
    nb_xc = (graph, col, (1 - x) * 2 + 1 - core)

    half_own = lax.rem(x + col, 2)
    half_far = 1 - half_own

    def position(half, side, sub):
        return pl.multiple_of(half * COLS + KC * (int(sub)) + SUB * side + int(SUB * (sub % 1)), HALF)

    def remote(ref_src, ref_dst, send, recv, dev):
        return pltpu.make_async_remote_copy(src_ref=ref_src, dst_ref=ref_dst, send_sem=send, recv_sem=recv,
                                            device_id=dev, device_id_type=MESH)

    cuts = (0, FIRST, 2 * FIRST, SUB, 2 * SUB, ROWS)
    loads = [pltpu.make_async_copy(g_hbm.at[pl.ds(lo, hi - lo)], g_f32.at[pl.ds(lo, hi - lo)], ld_sem.at[i])
             for i, (lo, hi) in enumerate(zip(cuts, cuts[1:]))]
    loads.append(pltpu.make_async_copy(a_hbm, a_f32, ld_sem.at[len(loads)]))
    for cp in loads:
        cp.start()

    barrier = pltpu.get_barrier_semaphore()
    for dev in (nb_x, nb_y, nb_c):
        pl.semaphore_signal(barrier, inc=1, device_id=dev, device_id_type=MESH)

    def rows(hc, half, side, sub, n=SUB):
        return G.at[hc, pl.ds(position(half, side, sub), n)]

    own_at = [rows(0, half_own, core, i) for i in range(NSUB)]
    gx_at = [rows(0, half_far, core, i) for i in range(NSUB)]
    gy_at = [rows(1, half_own, core, i) for i in range(NSUB)]
    dx_at = [rows(1, half_far, core, i) for i in range(NSUB)]
    tail_y = [rows(1, half_own, core, i, HALF) for i in TAIL]
    tail_d = [rows(1, half_far, core, i, HALF) for i in TAIL]

    gx_cp = [remote(own_at[i], own_at[i], snd.at[0], in_r.at[i // 2], nb_x) for i in range(NSUB)]
    def last_rows(hc, half, extra):
        first = half * COLS + KC * (NSUB - 1)
        if extra:
            return G.at[hc, pl.ds(pl.multiple_of(first + 2 * (SUB - LENT), 16), 2 * LENT)]
        return G.at[hc, pl.ds(pl.multiple_of(first + (SUB - LENT) * core, 16), SUB - LENT)]

    gy_cp = [remote(own_at[i], dx_at[i], snd.at[0], in_r.at[i // 2], nb_y) for i in range(NSUB - 1)]
    gy_cp += [remote(last_rows(0, half_own, e), last_rows(1, half_far, e), snd.at[3 if e else 0], in_r.at[1 + e], nb_y)
              for e in range(2)]
    dx_cp = [remote(at, at, snd.at[2], far_r.at[i], nb_x) for i, at in enumerate(gy_at[:-1] + tail_y)]
    c0_cp = [remote(at, at, snd.at[0], c0_r if i == NSUB - 1 else c01_r, nb_c) for i, at in enumerate(own_at)]
    c1_cp = [remote(at, at, snd.at[1], c01_r, nb_c) for at in gx_at]
    c2_cp = [remote(at, at, snd.at[1], c2_r, nb_c) for at in gy_at[:-1]]
    c2_cp += [remote(last_rows(1, half_own, e), last_rows(1, half_own, e), snd.at[3 if e else 1], c2x_r if e else c2_r, nb_c)
              for e in range(2)]
    c3_cp = [remote(at, at, snd.at[0], c3_r.at[min(i, NSUB - 1)], nb_c) for i, at in enumerate(dx_at[:-1] + tail_d)]
    ay_cp = [remote(A0.at[:, pl.ds(KC * n, KC)], A0.at[:, pl.ds(COLS + KC * n, KC)], snd.at[2], far_r.at[n if n < NKC - 1 else NSUB + 1], nb_y)
             for n in range(NKC)]

    def bytes_of(count, send, recv):
        at = G.at[0, pl.ds(0, count)] if count <= ORDER else G.at[:, pl.ds(0, count // 2)]
        return remote(at, at, send, recv, nb_c)

    def send_own(lo, hi):
        i = lo // SUB
        if hi - lo == SUB:
            gx_cp[i].start()
            if i < NSUB - 1:
                gy_cp[i].start()
            c0_cp[i].start()
        else:
            at = G.at[0, pl.ds(pl.multiple_of(position(half_own, core, 0) + lo, FIRST), hi - lo)]
            there = G.at[1, pl.ds(pl.multiple_of(position(half_far, core, 0) + lo, FIRST), hi - lo)]
            remote(at, at, snd.at[0], in_r.at[0], nb_x).start()
            remote(at, there, snd.at[0], in_r.at[0], nb_y).start()
            remote(at, at, snd.at[0], c01_r, nb_c).start()

    parts = (*zip(cuts, cuts[1:4]), *((SUB * i, SUB * (i + 1)) for i in range(1, NSUB)))
    for t, (lo, hi) in enumerate(parts):
        if lo in cuts:
            loads[cuts.index(lo)].wait()
        for b in range(8):
            p = place(b)
            G[0, pl.ds(pl.multiple_of(position(half_own, core, lo // SUB) + lo % SUB, FIRST), hi - lo), 128 * p:128 * p + 128] = (
                g_f32[lo:hi, 128 * b:128 * b + 128].astype(BF16))
        if t == 0:
            pl.semaphore_wait(barrier, 3)
        else:
            send_own(*parts[t - 1])
    loads[-1].wait()
    for b in range(8):
        p = place(b)
        A0[:, 128 * p:128 * p + 128] = a_f32[:, 128 * b:128 * b + 128].astype(BF16)
    send_own(*parts[-1])

    def dot(a, g):
        return jnp.dot(a, g, preferred_element_type=F32)

    c0_cp[-1].wait_recv()
    gy_cp[NSUB - 1].start()

    @pl.when(core == 1)
    def _():
        gy_cp[NSUB].start()

    for half in range(2):
        bytes_of(4 * SUB - half * LENT, snd.at[0], in_r.at[half]).wait_recv()
        for i in (2 * half, 2 * half + 1):
            c1_cp[i].start()
            c2_cp[i].start()
        if half == 0:
            for i in range(2):
                dx_cp[i].start()
                ay_cp[i].start()

    @pl.when(core == 1)
    def _():
        gy_cp[NSUB].wait_recv()
        c2_cp[NSUB].start()

    bytes_of(7 * SUB, snd.at[0], c01_r).wait_recv()
    C1[:, :COLS] = dot(A0[:, :COLS], G[0, :COLS, :])
    bytes_of(ROWS - LENT, snd.at[1], c2_r).wait_recv()

    @pl.when(core == 0)
    def _():
        c2_cp[NSUB].wait_recv()

    slots = []

    def share(it, lo, width, value):
        index = len(slots)
        slots.append(index)
        sums[it, 0, :, lo:lo + width] = value
        for r, dev in ((1, nb_c), (2, nb_x), (3, nb_xc)):
            remote(sums.at[it, 0, :, pl.ds(lo, width)], sums.at[it, r, :, pl.ds(lo, width)],
                   ar_s, ar_r.at[index], dev).start()
        return it, lo, width, index

    def three(it, lo, width, index):
        at = sums.at[it, pl.ds(1, 3), :, pl.ds(lo, width)]
        return remote(at, at, ar_s, ar_r.at[index], nb_c)

    def gathered(handle):
        it, lo, width, index = handle
        three(it, lo, width, index).wait_recv()
        s = [sums[it, r, :, lo:lo + width] for r in range(4)]
        return float(ORDER) / ((s[0] + s[1]) + (s[2] + s[3]))

    def square_and_share(it, dst, lo, width, value):
        m = value * value
        dst[:, lo:lo + width] = m
        return share(it, lo, width, jnp.sum(m, axis=0, keepdims=True))

    def rescale(dst, src, handle):
        f = gathered(handle)
        lo, width = handle[1:3]
        dst[:, lo:lo + width] = (src[:, lo:lo + width] * f).astype(BF16)

    def graph(lo, depth, first, width):
        return G[first // COLS, lo:lo + depth, first % COLS:first % COLS + width]

    def far_piece(i):
        dx_cp[i].wait_recv()
        c3_cp[i].start()

    bytes_of(3 * ROWS - LENT, snd.at[0], c2_r).wait_send()
    shared = []
    for n in range(NKC):
        if n < NKC - 1:
            bytes_of(2 * SUB, snd.at[0], far_r.at[n]).wait_recv()
            c3_cp[n].start()
        else:
            far_piece(n)
        for i in ((2,), (3, 4), (), ())[n]:
            dx_cp[i].start()
        if n + 2 < NKC:
            ay_cp[n + 2].start()
        if n == 2:
            bytes_of(2 * ROWS - LENT, snd.at[1], c2_r).wait_send()

            @pl.when(core == 1)
            def _():
                bytes_of(4 * LENT, snd.at[3], c2_r).wait_send()

        if n == NKC - 1:

            @pl.when(core == 1)
            def _():
                far_piece(NSUB)

            ay_cp[n].wait_recv()
        lo = KC * n
        hi = COLS + lo
        if n < NKC - 1:
            C1[:, :COLS] += dot(A0[:, hi:hi + KC], G[0, hi:hi + KC, :])
        else:
            for first, width in PIECES_1:
                if first < COLS:
                    v = C1[:, first:first + width] + dot(A0[:, hi:hi + KC], graph(hi, KC, first, width))
                    shared.append(square_and_share(0, C1, first, width, v))
                    if len(shared) == 1:

                        @pl.when(core == 0)
                        def _():
                            far_piece(NSUB)

        bytes_of(SUB, snd.at[0], c3_r.at[n]).wait_recv()
        for first, width in PIECES_1:
            if first < COLS:
                continue
            d = dot(A0[:, lo:lo + KC], graph(lo, KC, first, width)) + dot(A0[:, hi:hi + KC], graph(hi, KC, first, width))
            if n == 0:
                C1[:, first:first + width] = d
            elif n < NKC - 1:
                C1[:, first:first + width] += d
            else:
                shared.append(square_and_share(0, C1, first, width, C1[:, first:first + width] + d))

    bytes_of(2 * ROWS, snd.at[2], c2_r).wait_send()
    bytes_of(ROWS, snd.at[0], c2_r).wait_send()
    done = 0
    for t in range(1):
        rescale(A1, C1, shared[t])
        lo, depth = PIECES_1[t]
        for hc in range(2):
            at = slice(hc * COLS, (hc + 1) * COLS)
            d = dot(A1[:, lo:lo + depth], G[hc, lo:lo + depth, :])
            if t == 0:
                C2[:, at] = d
            else:
                C2[:, at] += d
        done = lo + depth
    rescale(A1, C1, shared[1])
    lo, depth = PIECES_1[1]
    for first, width in PIECES_2[:EARLY]:
        C2[:, first:first + width] += dot(A1[:, lo:lo + depth], graph(lo, depth, first, width))
    f = gathered(shared[2])
    three(0, 0, ORDER, 0).wait_send()
    shared = []
    held = None
    for t, (first, width) in enumerate(PIECES_2):
        v = C2[:, first:first + width]
        for lo, depth in PIECES_1[2 if t < EARLY else 1:]:
            for at in range(lo, lo + depth, STEP):
                if t == 0:
                    A1[:, at:at + STEP] = (C1[:, at:at + STEP] * f[:, at - lo:at - lo + STEP]).astype(BF16)
                v += dot(A1[:, at:at + STEP], graph(at, STEP, first, width))
                if held is not None:
                    shared.append(share(1, *held))
                    held = None
        m = v * v
        C2[:, first:first + width] = m
        held = first, width, jnp.sum(m, axis=0, keepdims=True)
    shared.append(share(1, *held))

    for t, (lo, depth) in enumerate(PIECES_2):
        rescale(A2, C2, shared[t])
        if t == len(PIECES_2) - 1:
            three(1, 0, ORDER, 0).wait_send()
        d = dot(A2[:, lo:lo + depth], G[0, lo:lo + depth, :])
        if t == 0:
            C1[:, :COLS] = d
        elif t < len(PIECES_2) - 1:
            C1[:, :COLS] += d
        else:
            v = C1[:, :COLS] + d
            m = v * v
            last = share(2, 0, COLS, jnp.sum(m, axis=0, keepdims=True))
            for b in range(8):
                p = place(b)
                m_ref[:, 128 * b:128 * b + 128] = m[:, 128 * p:128 * p + 128]
    f = gathered(last)
    for b in range(8):
        p = place(b)
        r_ref[:, 128 * b:128 * b + 128] = f[:, 128 * p:128 * p + 128]
    three(2, 0, COLS, 0).wait_send()


def scale_kernel(m_ref, r_ref, out_hbm, out, sem):
    factor = r_ref[...]
    step = ROWS // 8
    for i in range(8):
        at = pl.ds(step * i, step)
        out[at, :] = m_ref[at, :] * factor
        pltpu.make_async_copy(out.at[at], out_hbm.at[at], sem).start()
    pltpu.make_async_copy(out, out_hbm, sem).wait()


def solution(mesh):
    block_spec = P(("graph", "row"), "col")

    def device_step(init_blk, graph_blk):
        dma = pltpu.SemaphoreType.DMA
        in_hbm = [pltpu.with_memory_space_constraint(v, pltpu.HBM) for v in (init_blk, graph_blk)]
        m, r = pl.pallas_call(
            mcl_kernel,
            name="mcl",
            out_shape=(jax.ShapeDtypeStruct((ROWS, COLS), F32), jax.ShapeDtypeStruct((1, COLS), F32)),
            in_specs=[pl.BlockSpec(memory_space=pltpu.HBM)] * 2,
            out_specs=(pl.BlockSpec(memory_space=pltpu.VMEM),) * 2,
            scratch_shapes=[
                pltpu.VMEM((ROWS, COLS), F32),
                pltpu.VMEM((ROWS, COLS), F32),
                pltpu.VMEM((2, ORDER, COLS), BF16),
                pltpu.VMEM((ROWS, ORDER), BF16),
                pltpu.VMEM((ROWS, ORDER), BF16),
                pltpu.VMEM((ROWS, ORDER), BF16),
                pltpu.VMEM((ROWS, ORDER), F32),
                pltpu.VMEM((ROWS, ORDER), F32),
                pltpu.VMEM((3, 4, 1, ORDER), F32),
                dma((6,)), dma((4,)), dma((3,)), dma((NSUB + 2,)),
                dma(()), dma(()), dma(()), dma(()), dma((NSUB,)),
                dma(()), dma((len(PIECES_1) + len(PIECES_2) + 1,)),
            ],
            compiler_params=pltpu.CompilerParams(collective_id=0, has_side_effects=True, vmem_limit_bytes=48 * 2**20),
        )(*in_hbm)
        return pl.pallas_call(
            scale_kernel,
            name="scale",
            out_shape=jax.ShapeDtypeStruct((ROWS, COLS), F32),
            in_specs=[pl.BlockSpec(memory_space=pltpu.VMEM)] * 2,
            out_specs=pl.BlockSpec(memory_space=pltpu.HBM),
            scratch_shapes=[pltpu.VMEM((ROWS, COLS), F32), dma(())],
            compiler_params=pltpu.CompilerParams(vmem_limit_bytes=8 * 2**20),
        )(m, r)

    return jax.shard_map(device_step, mesh=mesh, in_specs=(block_spec, block_spec), out_specs=block_spec, check_vma=False)
```

```python
import jax
import jax.numpy as jnp
from jax import lax
from jax.experimental import pallas as pl
from jax.experimental.pallas import tpu as pltpu
from jax.sharding import PartitionSpec as P

MESH = pl.DeviceIdType.MESH
BF16 = jnp.bfloat16
F32 = jnp.float32

ROWS = 512
COLS = 1024
ORDER = 2048
SUB = 128
NSUB = ROWS // SUB
HALF = SUB // 2
FIRST = 32
LENT = 48
TAIL = (NSUB - 1, NSUB - 0.5)
KC = 256
NKC = COLS // KC
PIECES_1 = ((0, 512), (512, 512), (1024, 1024))
EARLY = 2
STEP = 512
PIECES_2 = ((1024, 512), (1536, 512), (0, 512), (512, 512))


def place(b):
    return 2 * (b % 4) + b // 4


def mcl_kernel(a_hbm, g_hbm, m_ref, r_ref,
               a_f32, g_f32, G, A0, A1, C1, C2, sums,
               ld_sem, snd, in_r, far_r, c0_r, c01_r, c2_r, c2x_r, c3_r, ar_s, ar_r):
    graph, col, row = lax.axis_index("graph"), lax.axis_index("col"), lax.axis_index("row")
    x, core = row // 2, row % 2
    nb_x = (graph, col, (1 - x) * 2 + core)
    nb_y = (graph, 1 - col, row)
    nb_c = (graph, col, x * 2 + 1 - core)
    nb_xc = (graph, col, (1 - x) * 2 + 1 - core)

    half_own = lax.rem(x + col, 2)
    half_far = 1 - half_own

    def position(half, side, sub):
        return pl.multiple_of(half * COLS + KC * (int(sub)) + SUB * side + int(SUB * (sub % 1)), HALF)

    def remote(ref_src, ref_dst, send, recv, dev):
        return pltpu.make_async_remote_copy(src_ref=ref_src, dst_ref=ref_dst, send_sem=send, recv_sem=recv,
                                            device_id=dev, device_id_type=MESH)

    cuts = (0, FIRST, 2 * FIRST, SUB, ROWS)
    loads = [pltpu.make_async_copy(g_hbm.at[pl.ds(lo, hi - lo)], g_f32.at[pl.ds(lo, hi - lo)], ld_sem.at[i])
             for i, (lo, hi) in enumerate(zip(cuts, cuts[1:]))]
    loads.append(pltpu.make_async_copy(a_hbm, a_f32, ld_sem.at[len(loads)]))
    for cp in loads:
        cp.start()

    barrier = pltpu.get_barrier_semaphore()
    for dev in (nb_x, nb_y, nb_c):
        pl.semaphore_signal(barrier, inc=1, device_id=dev, device_id_type=MESH)

    def rows(hc, half, side, sub, n=SUB):
        return G.at[hc, pl.ds(position(half, side, sub), n)]

    own_at = [rows(0, half_own, core, i) for i in range(NSUB)]
    gx_at = [rows(0, half_far, core, i) for i in range(NSUB)]
    gy_at = [rows(1, half_own, core, i) for i in range(NSUB)]
    dx_at = [rows(1, half_far, core, i) for i in range(NSUB)]
    tail_y = [rows(1, half_own, core, i, HALF) for i in TAIL]
    tail_d = [rows(1, half_far, core, i, HALF) for i in TAIL]

    gx_cp = [remote(own_at[i], own_at[i], snd.at[0], in_r.at[i // 2], nb_x) for i in range(NSUB)]
    def last_rows(hc, half, extra):
        first = half * COLS + KC * (NSUB - 1)
        if extra:
            return G.at[hc, pl.ds(pl.multiple_of(first + 2 * (SUB - LENT), 16), 2 * LENT)]
        return G.at[hc, pl.ds(pl.multiple_of(first + (SUB - LENT) * core, 16), SUB - LENT)]

    gy_cp = [remote(own_at[i], dx_at[i], snd.at[0], in_r.at[i // 2], nb_y) for i in range(NSUB - 1)]
    gy_cp += [remote(last_rows(0, half_own, e), last_rows(1, half_far, e), snd.at[3 if e else 0], in_r.at[1 + e], nb_y)
              for e in range(2)]
    dx_cp = [remote(at, at, snd.at[2], far_r.at[i], nb_x) for i, at in enumerate(gy_at[:-1] + tail_y)]
    c0_cp = [remote(at, at, snd.at[0], c0_r if i == NSUB - 1 else c01_r, nb_c) for i, at in enumerate(own_at)]
    c1_cp = [remote(at, at, snd.at[1], c01_r, nb_c) for at in gx_at]
    c2_cp = [remote(at, at, snd.at[1], c2_r, nb_c) for at in gy_at[:-1]]
    c2_cp += [remote(last_rows(1, half_own, e), last_rows(1, half_own, e), snd.at[3 if e else 1], c2x_r if e else c2_r, nb_c)
              for e in range(2)]
    c3_cp = [remote(at, at, snd.at[0], c3_r.at[0 if i < NSUB - 1 else 1], nb_c) for i, at in enumerate(dx_at[:-1] + tail_d)]
    ay_cp = [remote(A0.at[:, pl.ds(KC * n, KC)], A0.at[:, pl.ds(COLS + KC * n, KC)], snd.at[2], far_r.at[n if n < NKC - 1 else NSUB + 1], nb_y)
             for n in range(NKC)]

    def bytes_of(count, send, recv):
        at = G.at[0, pl.ds(0, count)] if count <= ORDER else G.at[:, pl.ds(0, count // 2)]
        return remote(at, at, send, recv, nb_c)

    def send_own(lo, hi):
        i = lo // SUB
        if hi - lo == SUB:
            gx_cp[i].start()
            if i < NSUB - 1:
                gy_cp[i].start()
            c0_cp[i].start()
        else:
            at = G.at[0, pl.ds(pl.multiple_of(position(half_own, core, 0) + lo, FIRST), hi - lo)]
            there = G.at[1, pl.ds(pl.multiple_of(position(half_far, core, 0) + lo, FIRST), hi - lo)]
            remote(at, at, snd.at[0], in_r.at[0], nb_x).start()
            remote(at, there, snd.at[0], in_r.at[0], nb_y).start()
            remote(at, at, snd.at[0], c01_r, nb_c).start()

    parts = (*zip(cuts, cuts[1:4]), *((SUB * i, SUB * (i + 1)) for i in range(1, NSUB)))
    for t, (lo, hi) in enumerate(parts):
        if lo in cuts:
            loads[cuts.index(lo)].wait()
        for b in range(8):
            p = place(b)
            G[0, pl.ds(pl.multiple_of(position(half_own, core, lo // SUB) + lo % SUB, FIRST), hi - lo), 128 * p:128 * p + 128] = (
                g_f32[lo:hi, 128 * b:128 * b + 128].astype(BF16))
        if t == 0:
            pl.semaphore_wait(barrier, 3)
        else:
            send_own(*parts[t - 1])
    loads[-1].wait()
    for b in range(8):
        p = place(b)
        A0[:, 128 * p:128 * p + 128] = a_f32[:, 128 * b:128 * b + 128].astype(BF16)
    send_own(*parts[-1])

    def dot(a, g):
        return jnp.dot(a, g, preferred_element_type=F32)

    c0_cp[-1].wait_recv()
    gy_cp[NSUB - 1].start()

    @pl.when(core == 1)
    def _():
        gy_cp[NSUB].start()

    for half in range(2):
        bytes_of(4 * SUB - half * LENT, snd.at[0], in_r.at[half]).wait_recv()
        for i in (2 * half, 2 * half + 1):
            c1_cp[i].start()
            c2_cp[i].start()
        if half == 0:
            for i in range(2):
                dx_cp[i].start()
                ay_cp[i].start()

    @pl.when(core == 1)
    def _():
        gy_cp[NSUB].wait_recv()
        c2_cp[NSUB].start()

    bytes_of(7 * SUB, snd.at[0], c01_r).wait_recv()
    C1[:, :COLS] = dot(A0[:, :COLS], G[0, :COLS, :])
    bytes_of(ROWS - LENT, snd.at[1], c2_r).wait_recv()

    @pl.when(core == 0)
    def _():
        c2_cp[NSUB].wait_recv()

    slots = []

    def share(it, lo, width, value):
        index = len(slots)
        slots.append(index)
        sums[it, 0, :, lo:lo + width] = value
        for r, dev in ((1, nb_c), (2, nb_x), (3, nb_xc)):
            remote(sums.at[it, 0, :, pl.ds(lo, width)], sums.at[it, r, :, pl.ds(lo, width)],
                   ar_s, ar_r.at[index], dev).start()
        return it, lo, width, index

    def three(it, lo, width, index):
        at = sums.at[it, pl.ds(1, 3), :, pl.ds(lo, width)]
        return remote(at, at, ar_s, ar_r.at[index], nb_c)

    def gathered(handle):
        it, lo, width, index = handle
        three(it, lo, width, index).wait_recv()
        s = [sums[it, r, :, lo:lo + width] for r in range(4)]
        return float(ORDER) / ((s[0] + s[1]) + (s[2] + s[3]))

    def square_and_share(it, dst, lo, width, value):
        m = value * value
        dst[:, lo:lo + width] = m
        return share(it, lo, width, jnp.sum(m, axis=0, keepdims=True))

    def rescale(dst, src, handle):
        f = gathered(handle)
        lo, width = handle[1:3]
        dst[:, lo:lo + width] = (src[:, lo:lo + width] * f).astype(BF16)

    def graph(lo, depth, first, width):
        return G[first // COLS, lo:lo + depth, first % COLS:first % COLS + width]

    def far_piece(i):
        dx_cp[i].wait_recv()
        c3_cp[i].start()

    bytes_of(3 * ROWS - LENT, snd.at[0], c2_r).wait_send()
    shared = []
    for n in range(NKC):
        if n < NKC - 1:
            bytes_of(2 * SUB, snd.at[0], far_r.at[n]).wait_recv()
            c3_cp[n].start()
        else:
            far_piece(n)
        for i in ((2,), (3, 4), (), ())[n]:
            dx_cp[i].start()
        if n + 2 < NKC:
            ay_cp[n + 2].start()
        if n == 2:
            bytes_of(2 * ROWS - LENT, snd.at[1], c2_r).wait_send()

            @pl.when(core == 1)
            def _():
                bytes_of(4 * LENT, snd.at[3], c2_r).wait_send()

        if n == NKC - 1:

            @pl.when(core == 1)
            def _():
                far_piece(NSUB)

            ay_cp[n].wait_recv()
        lo = KC * n
        hi = COLS + lo
        if n < NKC - 1:
            C1[:, :COLS] += dot(A0[:, hi:hi + KC], G[0, hi:hi + KC, :])
        else:
            for first, width in PIECES_1:
                if first < COLS:
                    v = C1[:, first:first + width] + dot(A0[:, hi:hi + KC], graph(hi, KC, first, width))
                    shared.append(square_and_share(0, C1, first, width, v))
                    if len(shared) == 1:

                        @pl.when(core == 0)
                        def _():
                            far_piece(NSUB)

        if n < 2:
            continue
        bytes_of(SUB * (3 if n == 2 else 1), snd.at[0], c3_r.at[n - 2]).wait_recv()
        for first, width in PIECES_1:
            if first < COLS:
                continue
            if n == 2:
                C1[:, first:first + width] = (dot(A0[:, :hi - COLS + KC], graph(0, lo + KC, first, width))
                                              + dot(A0[:, COLS:hi + KC], graph(COLS, lo + KC, first, width)))
            else:
                d = dot(A0[:, lo:lo + KC], graph(lo, KC, first, width)) + dot(A0[:, hi:hi + KC], graph(hi, KC, first, width))
                shared.append(square_and_share(0, C1, first, width, C1[:, first:first + width] + d))

    bytes_of(2 * ROWS, snd.at[2], c2_r).wait_send()
    bytes_of(ROWS, snd.at[0], c2_r).wait_send()
    lo, depth = PIECES_1[0]
    a = (C1[:, lo:lo + depth] * gathered(shared[0])).astype(BF16)
    for hc in range(2):
        C2[:, hc * COLS:(hc + 1) * COLS] = dot(a, G[hc, lo:lo + depth, :])
    rescale(A1, C1, shared[1])
    lo, depth = PIECES_1[1]
    for first, width in PIECES_2[:EARLY]:
        C2[:, first:first + width] += dot(A1[:, lo:lo + depth], graph(lo, depth, first, width))
    f = gathered(shared[2])
    three(0, 0, ORDER, 0).wait_send()
    shared = []
    held = None
    for t, (first, width) in enumerate(PIECES_2):
        v = C2[:, first:first + width]
        for lo, depth in PIECES_1[2 if t < EARLY else 1:]:
            for at in range(lo, lo + depth, STEP):
                if t == 0:
                    A1[:, at:at + STEP] = (C1[:, at:at + STEP] * f[:, at - lo:at - lo + STEP]).astype(BF16)
                v += dot(A1[:, at:at + STEP], graph(at, STEP, first, width))
                if held is not None:
                    shared.append(share(1, *held))
                    held = None
        m = v * v
        C2[:, first:first + width] = m
        held = first, width, jnp.sum(m, axis=0, keepdims=True)
    shared.append(share(1, *held))

    for t, (lo, depth) in enumerate(PIECES_2):
        f = gathered(shared[t])
        if t == len(PIECES_2) - 1:
            three(1, 0, ORDER, 0).wait_send()
        d = dot((C2[:, lo:lo + depth] * f).astype(BF16), G[0, lo:lo + depth, :])
        if t == 0:
            C1[:, :COLS] = d
        elif t < len(PIECES_2) - 1:
            C1[:, :COLS] += d
        else:
            v = C1[:, :COLS] + d
            m = v * v
            last = share(2, 0, COLS, jnp.sum(m, axis=0, keepdims=True))
            for b in range(8):
                p = place(b)
                m_ref[:, 128 * b:128 * b + 128] = m[:, 128 * p:128 * p + 128]
    f = gathered(last)
    for b in range(8):
        p = place(b)
        r_ref[:, 128 * b:128 * b + 128] = f[:, 128 * p:128 * p + 128]
    three(2, 0, COLS, 0).wait_send()


def scale_kernel(m_ref, r_ref, out_hbm, out, sem):
    factor = r_ref[...]
    step = ROWS // 8
    for i in range(8):
        at = pl.ds(step * i, step)
        out[at, :] = m_ref[at, :] * factor
        pltpu.make_async_copy(out.at[at], out_hbm.at[at], sem).start()
    pltpu.make_async_copy(out, out_hbm, sem).wait()


def solution(mesh):
    block_spec = P(("graph", "row"), "col")

    def device_step(init_blk, graph_blk):
        dma = pltpu.SemaphoreType.DMA
        in_hbm = [pltpu.with_memory_space_constraint(v, pltpu.HBM) for v in (init_blk, graph_blk)]
        m, r = pl.pallas_call(
            mcl_kernel,
            name="mcl",
            out_shape=(jax.ShapeDtypeStruct((ROWS, COLS), F32), jax.ShapeDtypeStruct((1, COLS), F32)),
            in_specs=[pl.BlockSpec(memory_space=pltpu.HBM)] * 2,
            out_specs=(pl.BlockSpec(memory_space=pltpu.VMEM),) * 2,
            scratch_shapes=[
                pltpu.VMEM((ROWS, COLS), F32),
                pltpu.VMEM((ROWS, COLS), F32),
                pltpu.VMEM((2, ORDER, COLS), BF16),
                pltpu.VMEM((ROWS, ORDER), BF16),
                pltpu.VMEM((ROWS, ORDER), BF16),
                pltpu.VMEM((ROWS, ORDER), F32),
                pltpu.VMEM((ROWS, ORDER), F32),
                pltpu.VMEM((3, 4, 1, ORDER), F32),
                dma((5,)), dma((4,)), dma((3,)), dma((NSUB + 2,)),
                dma(()), dma(()), dma(()), dma(()), dma((2,)),
                dma(()), dma((len(PIECES_1) + len(PIECES_2) + 1,)),
            ],
            compiler_params=pltpu.CompilerParams(collective_id=0, has_side_effects=True, vmem_limit_bytes=48 * 2**20),
        )(*in_hbm)
        return pl.pallas_call(
            scale_kernel,
            name="scale",
            out_shape=jax.ShapeDtypeStruct((ROWS, COLS), F32),
            in_specs=[pl.BlockSpec(memory_space=pltpu.VMEM)] * 2,
            out_specs=pl.BlockSpec(memory_space=pltpu.HBM),
            scratch_shapes=[pltpu.VMEM((ROWS, COLS), F32), dma(())],
            compiler_params=pltpu.CompilerParams(vmem_limit_bytes=8 * 2**20),
        )(m, r)

    return jax.shard_map(device_step, mesh=mesh, in_specs=(block_spec, block_spec), out_specs=block_spec, check_vma=False)
```

```python
import jax
import jax.numpy as jnp
from jax import lax
from jax.experimental import pallas as pl
from jax.experimental.pallas import tpu as pltpu
from jax.sharding import PartitionSpec as P

MESH = pl.DeviceIdType.MESH
BF16 = jnp.bfloat16
F32 = jnp.float32

ROWS = 512
COLS = 1024
ORDER = 2048
SUB = 128
NSUB = ROWS // SUB
HALF = SUB // 2
FIRST = 32
LENT = 48
TAIL = (NSUB - 1, NSUB - 0.5)
KC = 256
NKC = COLS // KC
PIECES_1 = ((0, 512), (512, 512), (1024, 1024))
EARLY = 2
STEP = 512
PIECES_2 = ((1024, 512), (1536, 512), (0, 512), (512, 512))


def place(b):
    return 2 * (b % 4) + b // 4


def mcl_kernel(a_hbm, g_hbm, m_ref, r_ref,
               a_f32, g_f32, G, A0, A1, C1, C2, sums,
               ld_sem, snd, in_r, far_r, c0_r, c01_r, c2_r, c2x_r, c3_r, ar_s, ar_r):
    graph, col, row = lax.axis_index("graph"), lax.axis_index("col"), lax.axis_index("row")
    x, core = row // 2, row % 2
    nb_x = (graph, col, (1 - x) * 2 + core)
    nb_y = (graph, 1 - col, row)
    nb_c = (graph, col, x * 2 + 1 - core)
    nb_xc = (graph, col, (1 - x) * 2 + 1 - core)

    half_own = lax.rem(x + col, 2)
    half_far = 1 - half_own

    def position(half, side, sub):
        return pl.multiple_of(half * COLS + KC * (int(sub)) + SUB * side + int(SUB * (sub % 1)), HALF)

    def remote(ref_src, ref_dst, send, recv, dev):
        return pltpu.make_async_remote_copy(src_ref=ref_src, dst_ref=ref_dst, send_sem=send, recv_sem=recv,
                                            device_id=dev, device_id_type=MESH)

    cuts = (0, FIRST, 2 * FIRST, ROWS)
    loads = [pltpu.make_async_copy(g_hbm.at[pl.ds(lo, hi - lo)], g_f32.at[pl.ds(lo, hi - lo)], ld_sem.at[i])
             for i, (lo, hi) in enumerate(zip(cuts, cuts[1:]))]
    loads.append(pltpu.make_async_copy(a_hbm, a_f32, ld_sem.at[len(loads)]))
    for cp in loads:
        cp.start()

    barrier = pltpu.get_barrier_semaphore()
    for dev in (nb_x, nb_y, nb_c):
        pl.semaphore_signal(barrier, inc=1, device_id=dev, device_id_type=MESH)

    def rows(hc, half, side, sub, n=SUB):
        return G.at[hc, pl.ds(position(half, side, sub), n)]

    own_at = [rows(0, half_own, core, i) for i in range(NSUB)]
    gx_at = [rows(0, half_far, core, i) for i in range(NSUB)]
    gy_at = [rows(1, half_own, core, i) for i in range(NSUB)]
    dx_at = [rows(1, half_far, core, i) for i in range(NSUB)]
    tail_y = [rows(1, half_own, core, i, HALF) for i in TAIL]
    tail_d = [rows(1, half_far, core, i, HALF) for i in TAIL]

    gx_cp = [remote(own_at[i], own_at[i], snd.at[0], in_r.at[i // 2], nb_x) for i in range(NSUB)]
    def last_rows(hc, half, extra):
        first = half * COLS + KC * (NSUB - 1)
        if extra:
            return G.at[hc, pl.ds(pl.multiple_of(first + 2 * (SUB - LENT), 16), 2 * LENT)]
        return G.at[hc, pl.ds(pl.multiple_of(first + (SUB - LENT) * core, 16), SUB - LENT)]

    gy_cp = [remote(own_at[i], dx_at[i], snd.at[0], in_r.at[i // 2], nb_y) for i in range(NSUB - 1)]
    gy_cp += [remote(last_rows(0, half_own, e), last_rows(1, half_far, e), snd.at[3 if e else 0], in_r.at[1 + e], nb_y)
              for e in range(2)]
    dx_cp = [remote(at, at, snd.at[2], far_r.at[i], nb_x) for i, at in enumerate(gy_at[:-1] + tail_y)]
    c0_cp = [remote(at, at, snd.at[0], c0_r if i == NSUB - 1 else c01_r, nb_c) for i, at in enumerate(own_at)]
    c1_cp = [remote(at, at, snd.at[1], c01_r, nb_c) for at in gx_at]
    c2_cp = [remote(at, at, snd.at[1], c2_r, nb_c) for at in gy_at[:-1]]
    c2_cp += [remote(last_rows(1, half_own, e), last_rows(1, half_own, e), snd.at[3 if e else 1], c2x_r if e else c2_r, nb_c)
              for e in range(2)]
    c3_cp = [remote(at, at, snd.at[0], c3_r.at[0 if i < NSUB - 1 else 1], nb_c) for i, at in enumerate(dx_at[:-1] + tail_d)]
    ay_cp = [remote(A0.at[:, pl.ds(KC * n, KC)], A0.at[:, pl.ds(COLS + KC * n, KC)], snd.at[2], far_r.at[n if n < NKC - 1 else NSUB + 1], nb_y)
             for n in range(NKC)]

    def bytes_of(count, send, recv):
        at = G.at[0, pl.ds(0, count)] if count <= ORDER else G.at[:, pl.ds(0, count // 2)]
        return remote(at, at, send, recv, nb_c)

    def send_own(lo, hi):
        i = lo // SUB
        if hi - lo == SUB:
            gx_cp[i].start()
            if i < NSUB - 1:
                gy_cp[i].start()
            c0_cp[i].start()
        else:
            at = G.at[0, pl.ds(pl.multiple_of(position(half_own, core, 0) + lo, FIRST), hi - lo)]
            there = G.at[1, pl.ds(pl.multiple_of(position(half_far, core, 0) + lo, FIRST), hi - lo)]
            remote(at, at, snd.at[0], in_r.at[0], nb_x).start()
            remote(at, there, snd.at[0], in_r.at[0], nb_y).start()
            remote(at, at, snd.at[0], c01_r, nb_c).start()

    parts = (*zip((0, FIRST, 2 * FIRST), (FIRST, 2 * FIRST, SUB)), *((SUB * i, SUB * (i + 1)) for i in range(1, NSUB)))
    for t, (lo, hi) in enumerate(parts):
        if lo in cuts:
            loads[cuts.index(lo)].wait()
        for b in range(8):
            p = place(b)
            G[0, pl.ds(pl.multiple_of(position(half_own, core, lo // SUB) + lo % SUB, FIRST), hi - lo), 128 * p:128 * p + 128] = (
                g_f32[lo:hi, 128 * b:128 * b + 128].astype(BF16))
        if t == 0:
            pl.semaphore_wait(barrier, 3)
        else:
            send_own(*parts[t - 1])
    loads[-1].wait()
    for b in range(8):
        p = place(b)
        A0[:, 128 * p:128 * p + 128] = a_f32[:, 128 * b:128 * b + 128].astype(BF16)
    send_own(*parts[-1])

    def dot(a, g):
        return jnp.dot(a, g, preferred_element_type=F32)

    c0_cp[-1].wait_recv()
    gy_cp[NSUB - 1].start()

    @pl.when(core == 1)
    def _():
        gy_cp[NSUB].start()

    for half in range(2):
        bytes_of(4 * SUB - half * LENT, snd.at[0], in_r.at[half]).wait_recv()
        for i in (2 * half, 2 * half + 1):
            c1_cp[i].start()
            c2_cp[i].start()
        if half == 0:
            for i in range(2):
                dx_cp[i].start()
                ay_cp[i].start()

    @pl.when(core == 1)
    def _():
        gy_cp[NSUB].wait_recv()
        c2_cp[NSUB].start()

    bytes_of(7 * SUB, snd.at[0], c01_r).wait_recv()
    C1[:, :COLS] = dot(A0[:, :COLS], G[0, :COLS, :])
    bytes_of(ROWS - LENT, snd.at[1], c2_r).wait_recv()

    @pl.when(core == 0)
    def _():
        c2_cp[NSUB].wait_recv()

    slots = []

    def share(it, lo, width, value):
        index = len(slots)
        slots.append(index)
        sums[it, 0, :, lo:lo + width] = value
        for r, dev in ((1, nb_c), (2, nb_x), (3, nb_xc)):
            remote(sums.at[it, 0, :, pl.ds(lo, width)], sums.at[it, r, :, pl.ds(lo, width)],
                   ar_s, ar_r.at[index], dev).start()
        return it, lo, width, index

    def three(it, lo, width, index):
        at = sums.at[it, pl.ds(1, 3), :, pl.ds(lo, width)]
        return remote(at, at, ar_s, ar_r.at[index], nb_c)

    def gathered(handle):
        it, lo, width, index = handle
        three(it, lo, width, index).wait_recv()
        s = [sums[it, r, :, lo:lo + width] for r in range(4)]
        return float(ORDER) / ((s[0] + s[1]) + (s[2] + s[3]))

    def square_and_share(it, dst, lo, width, value):
        m = value * value
        dst[:, lo:lo + width] = m
        return share(it, lo, width, jnp.sum(m, axis=0, keepdims=True))

    def rescale(dst, src, handle):
        f = gathered(handle)
        lo, width = handle[1:3]
        dst[:, lo:lo + width] = (src[:, lo:lo + width] * f).astype(BF16)

    def graph(lo, depth, first, width):
        return G[first // COLS, lo:lo + depth, first % COLS:first % COLS + width]

    def far_piece(i):
        dx_cp[i].wait_recv()
        c3_cp[i].start()

    bytes_of(3 * ROWS - LENT, snd.at[0], c2_r).wait_send()
    shared = []
    for n in range(NKC):
        if n < NKC - 1:
            bytes_of(2 * SUB, snd.at[0], far_r.at[n]).wait_recv()
            c3_cp[n].start()
        else:
            far_piece(n)
        for i in ((2,), (3, 4), (), ())[n]:
            dx_cp[i].start()
        if n + 2 < NKC:
            ay_cp[n + 2].start()
        if n == 2:
            bytes_of(2 * ROWS - LENT, snd.at[1], c2_r).wait_send()

            @pl.when(core == 1)
            def _():
                bytes_of(4 * LENT, snd.at[3], c2_r).wait_send()

        if n == NKC - 1:

            @pl.when(core == 1)
            def _():
                far_piece(NSUB)

            ay_cp[n].wait_recv()
        lo = KC * n
        hi = COLS + lo
        if n < NKC - 1:
            C1[:, :COLS] += dot(A0[:, hi:hi + KC], G[0, hi:hi + KC, :])
        else:
            for first, width in PIECES_1:
                if first < COLS:
                    v = C1[:, first:first + width] + dot(A0[:, hi:hi + KC], graph(hi, KC, first, width))
                    shared.append(square_and_share(0, C1, first, width, v))
                    if len(shared) == 1:

                        @pl.when(core == 0)
                        def _():
                            far_piece(NSUB)

        if n < 2:
            continue
        bytes_of(SUB * (3 if n == 2 else 1), snd.at[0], c3_r.at[n - 2]).wait_recv()
        for first, width in PIECES_1:
            if first < COLS:
                continue
            if n == 2:
                C1[:, first:first + width] = (dot(A0[:, :hi - COLS + KC], graph(0, lo + KC, first, width))
                                              + dot(A0[:, COLS:hi + KC], graph(COLS, lo + KC, first, width)))
            else:
                d = dot(A0[:, lo:lo + KC], graph(lo, KC, first, width)) + dot(A0[:, hi:hi + KC], graph(hi, KC, first, width))
                shared.append(square_and_share(0, C1, first, width, C1[:, first:first + width] + d))

    bytes_of(2 * ROWS, snd.at[2], c2_r).wait_send()
    bytes_of(ROWS, snd.at[0], c2_r).wait_send()
    lo, depth = PIECES_1[0]
    a = (C1[:, lo:lo + depth] * gathered(shared[0])).astype(BF16)
    for hc in range(2):
        C2[:, hc * COLS:(hc + 1) * COLS] = dot(a, G[hc, lo:lo + depth, :])
    rescale(A1, C1, shared[1])
    lo, depth = PIECES_1[1]
    for first, width in PIECES_2[:EARLY]:
        C2[:, first:first + width] += dot(A1[:, lo:lo + depth], graph(lo, depth, first, width))
    f = gathered(shared[2])
    three(0, 0, ORDER, 0).wait_send()
    shared = []
    held = None
    for t, (first, width) in enumerate(PIECES_2):
        v = C2[:, first:first + width]
        for lo, depth in PIECES_1[2 if t < EARLY else 1:]:
            for at in range(lo, lo + depth, STEP):
                if t == 0:
                    A1[:, at:at + STEP] = (C1[:, at:at + STEP] * f[:, at - lo:at - lo + STEP]).astype(BF16)
                v += dot(A1[:, at:at + STEP], graph(at, STEP, first, width))
                if held is not None:
                    shared.append(share(1, *held))
                    held = None
        m = v * v
        C2[:, first:first + width] = m
        held = first, width, jnp.sum(m, axis=0, keepdims=True)
    shared.append(share(1, *held))

    for t, (lo, depth) in enumerate(PIECES_2):
        f = gathered(shared[t])
        if t == len(PIECES_2) - 1:
            three(1, 0, ORDER, 0).wait_send()
        d = dot((C2[:, lo:lo + depth] * f).astype(BF16), G[0, lo:lo + depth, :])
        if t == 0:
            C1[:, :COLS] = d
        elif t < len(PIECES_2) - 1:
            C1[:, :COLS] += d
        else:
            v = C1[:, :COLS] + d
            m = v * v
            last = share(2, 0, COLS, jnp.sum(m, axis=0, keepdims=True))
            for b in range(8):
                p = place(b)
                m_ref[:, 128 * b:128 * b + 128] = m[:, 128 * p:128 * p + 128]
    f = gathered(last)
    for b in range(8):
        p = place(b)
        r_ref[:, 128 * b:128 * b + 128] = f[:, 128 * p:128 * p + 128]
    three(2, 0, COLS, 0).wait_send()


def scale_kernel(m_ref, r_ref, out_hbm, out, sem):
    factor = r_ref[...]
    step = ROWS // 16
    for i in range(16):
        at = pl.ds(step * i, step)
        out[at, :] = m_ref[at, :] * factor
        pltpu.make_async_copy(out.at[at], out_hbm.at[at], sem).start()
    pltpu.make_async_copy(out, out_hbm, sem).wait()


def solution(mesh):
    block_spec = P(("graph", "row"), "col")

    def device_step(init_blk, graph_blk):
        dma = pltpu.SemaphoreType.DMA
        in_hbm = [pltpu.with_memory_space_constraint(v, pltpu.HBM) for v in (init_blk, graph_blk)]
        m, r = pl.pallas_call(
            mcl_kernel,
            name="mcl",
            out_shape=(jax.ShapeDtypeStruct((ROWS, COLS), F32), jax.ShapeDtypeStruct((1, COLS), F32)),
            in_specs=[pl.BlockSpec(memory_space=pltpu.HBM)] * 2,
            out_specs=(pl.BlockSpec(memory_space=pltpu.VMEM),) * 2,
            scratch_shapes=[
                pltpu.VMEM((ROWS, COLS), F32),
                pltpu.VMEM((ROWS, COLS), F32),
                pltpu.VMEM((2, ORDER, COLS), BF16),
                pltpu.VMEM((ROWS, ORDER), BF16),
                pltpu.VMEM((ROWS, ORDER), BF16),
                pltpu.VMEM((ROWS, ORDER), F32),
                pltpu.VMEM((ROWS, ORDER), F32),
                pltpu.VMEM((3, 4, 1, ORDER), F32),
                dma((4,)), dma((4,)), dma((3,)), dma((NSUB + 2,)),
                dma(()), dma(()), dma(()), dma(()), dma((2,)),
                dma(()), dma((len(PIECES_1) + len(PIECES_2) + 1,)),
            ],
            compiler_params=pltpu.CompilerParams(collective_id=0, has_side_effects=True, vmem_limit_bytes=48 * 2**20),
        )(*in_hbm)
        return pl.pallas_call(
            scale_kernel,
            name="scale",
            out_shape=jax.ShapeDtypeStruct((ROWS, COLS), F32),
            in_specs=[pl.BlockSpec(memory_space=pltpu.VMEM)] * 2,
            out_specs=pl.BlockSpec(memory_space=pltpu.HBM),
            scratch_shapes=[pltpu.VMEM((ROWS, COLS), F32), dma(())],
            compiler_params=pltpu.CompilerParams(vmem_limit_bytes=8 * 2**20),
        )(m, r)

    return jax.shard_map(device_step, mesh=mesh, in_specs=(block_spec, block_spec), out_specs=block_spec, check_vma=False)
```

```python
import jax
import jax.numpy as jnp
from jax import lax
from jax.experimental import pallas as pl
from jax.experimental.pallas import tpu as pltpu
from jax.sharding import PartitionSpec as P

MESH = pl.DeviceIdType.MESH
BF16 = jnp.bfloat16
F32 = jnp.float32

ROWS = 512
COLS = 1024
ORDER = 2048
SUB = 128
NSUB = ROWS // SUB
HALF = SUB // 2
FIRST = 32
LENT = 48
TAIL = (NSUB - 1, NSUB - 0.5)
KC = 256
NKC = COLS // KC
PIECES_1 = ((0, 512), (512, 512), (1024, 1024))
EARLY = 2
STEP = 512
PIECES_2 = ((1024, 512), (1536, 512), (0, 512), (512, 512))


def place(b):
    return 2 * (b % 4) + b // 4


def mcl_kernel(a_hbm, g_hbm, m_ref, r_ref,
               a_f32, g_f32, G, A0, A1, C1, C2, sums,
               ld_sem, snd, in_r, far_r, c0_r, c01_r, c2_r, c2x_r, c3_r, ar_s, ar_r):
    graph, col, row = lax.axis_index("graph"), lax.axis_index("col"), lax.axis_index("row")
    x, core = row // 2, row % 2
    nb_x = (graph, col, (1 - x) * 2 + core)
    nb_y = (graph, 1 - col, row)
    nb_c = (graph, col, x * 2 + 1 - core)
    nb_xc = (graph, col, (1 - x) * 2 + 1 - core)

    half_own = lax.rem(x + col, 2)
    half_far = 1 - half_own

    def position(half, side, sub):
        return pl.multiple_of(half * COLS + KC * (int(sub)) + SUB * side + int(SUB * (sub % 1)), HALF)

    def remote(ref_src, ref_dst, send, recv, dev):
        return pltpu.make_async_remote_copy(src_ref=ref_src, dst_ref=ref_dst, send_sem=send, recv_sem=recv,
                                            device_id=dev, device_id_type=MESH)

    cuts = (0, FIRST, 2 * FIRST, ROWS)
    loads = [pltpu.make_async_copy(g_hbm.at[pl.ds(lo, hi - lo)], g_f32.at[pl.ds(lo, hi - lo)], ld_sem.at[i])
             for i, (lo, hi) in enumerate(zip(cuts, cuts[1:]))]
    loads.append(pltpu.make_async_copy(a_hbm, a_f32, ld_sem.at[len(loads)]))
    for cp in loads:
        cp.start()

    barrier = pltpu.get_barrier_semaphore()
    for dev in (nb_x, nb_y, nb_c):
        pl.semaphore_signal(barrier, inc=1, device_id=dev, device_id_type=MESH)

    def rows(hc, half, side, sub, n=SUB):
        return G.at[hc, pl.ds(position(half, side, sub), n)]

    own_at = [rows(0, half_own, core, i) for i in range(NSUB)]
    gx_at = [rows(0, half_far, core, i) for i in range(NSUB)]
    gy_at = [rows(1, half_own, core, i) for i in range(NSUB)]
    dx_at = [rows(1, half_far, core, i) for i in range(NSUB)]
    tail_y = [rows(1, half_own, core, i, HALF) for i in TAIL]
    tail_d = [rows(1, half_far, core, i, HALF) for i in TAIL]

    gx_cp = [remote(own_at[i], own_at[i], snd.at[0], in_r.at[i // 2], nb_x) for i in range(NSUB)]
    def last_rows(hc, half, extra):
        first = half * COLS + KC * (NSUB - 1)
        if extra:
            return G.at[hc, pl.ds(pl.multiple_of(first + 2 * (SUB - LENT), 16), 2 * LENT)]
        return G.at[hc, pl.ds(pl.multiple_of(first + (SUB - LENT) * core, 16), SUB - LENT)]

    gy_cp = [remote(own_at[i], dx_at[i], snd.at[0], in_r.at[i // 2], nb_y) for i in range(NSUB - 1)]
    gy_cp += [remote(last_rows(0, half_own, e), last_rows(1, half_far, e), snd.at[3 if e else 0], in_r.at[1 + e], nb_y)
              for e in range(2)]
    dx_cp = [remote(at, at, snd.at[2], far_r.at[i], nb_x) for i, at in enumerate(gy_at[:-1] + tail_y)]
    c0_cp = [remote(at, at, snd.at[0], c0_r if i == NSUB - 1 else c01_r, nb_c) for i, at in enumerate(own_at)]
    c1_cp = [remote(at, at, snd.at[1], c01_r, nb_c) for at in gx_at]
    c2_cp = [remote(at, at, snd.at[1], c2_r, nb_c) for at in gy_at[:-1]]
    c2_cp += [remote(last_rows(1, half_own, e), last_rows(1, half_own, e), snd.at[3 if e else 1], c2x_r if e else c2_r, nb_c)
              for e in range(2)]
    c3_cp = [remote(at, at, snd.at[0], c3_r.at[0 if i < NSUB - 1 else 1], nb_c) for i, at in enumerate(dx_at[:-1] + tail_d)]
    ay_cp = [remote(A0.at[:, pl.ds(KC * n, KC)], A0.at[:, pl.ds(COLS + KC * n, KC)], snd.at[2], far_r.at[n if n < NKC - 1 else NSUB + 1], nb_y)
             for n in range(NKC)]

    def bytes_of(count, send, recv):
        at = G.at[0, pl.ds(0, count)] if count <= ORDER else G.at[:, pl.ds(0, count // 2)]
        return remote(at, at, send, recv, nb_c)

    def send_own(lo, hi):
        i = lo // SUB
        if hi - lo == SUB:
            gx_cp[i].start()
            if i < NSUB - 1:
                gy_cp[i].start()
            c0_cp[i].start()
        else:
            at = G.at[0, pl.ds(pl.multiple_of(position(half_own, core, 0) + lo, FIRST), hi - lo)]
            there = G.at[1, pl.ds(pl.multiple_of(position(half_far, core, 0) + lo, FIRST), hi - lo)]
            remote(at, at, snd.at[0], in_r.at[0], nb_x).start()
            remote(at, there, snd.at[0], in_r.at[0], nb_y).start()
            remote(at, at, snd.at[0], c01_r, nb_c).start()

    parts = (*zip((0, FIRST, 2 * FIRST), (FIRST, 2 * FIRST, SUB)), *((SUB * i, SUB * (i + 1)) for i in range(1, NSUB)))
    for t, (lo, hi) in enumerate(parts):
        if lo in cuts:
            loads[cuts.index(lo)].wait()
        for b in range(8):
            p = place(b)
            G[0, pl.ds(pl.multiple_of(position(half_own, core, lo // SUB) + lo % SUB, FIRST), hi - lo), 128 * p:128 * p + 128] = (
                g_f32[lo:hi, 128 * b:128 * b + 128].astype(BF16))
        if t == 0:
            pl.semaphore_wait(barrier, 3)
        else:
            send_own(*parts[t - 1])
    loads[-1].wait()
    for b in range(8):
        p = place(b)
        A0[:, 128 * p:128 * p + 128] = a_f32[:, 128 * b:128 * b + 128].astype(BF16)
    send_own(*parts[-1])

    def dot(a, g):
        return jnp.dot(a, g, preferred_element_type=F32)

    c0_cp[-1].wait_recv()
    gy_cp[NSUB - 1].start()

    @pl.when(core == 1)
    def _():
        gy_cp[NSUB].start()

    for half in range(2):
        bytes_of(4 * SUB - half * LENT, snd.at[0], in_r.at[half]).wait_recv()
        for i in (2 * half, 2 * half + 1):
            c1_cp[i].start()
            c2_cp[i].start()
        if half == 0:
            for i in range(2):
                dx_cp[i].start()
                ay_cp[i].start()

    @pl.when(core == 1)
    def _():
        gy_cp[NSUB].wait_recv()
        c2_cp[NSUB].start()

    bytes_of(7 * SUB, snd.at[0], c01_r).wait_recv()
    C1[:, :COLS] = dot(A0[:, :COLS], G[0, :COLS, :])
    bytes_of(ROWS - LENT, snd.at[1], c2_r).wait_recv()

    @pl.when(core == 0)
    def _():
        c2_cp[NSUB].wait_recv()

    slots = []

    def share(it, lo, width, value):
        index = len(slots)
        slots.append(index)
        sums[it, 0, :, lo:lo + width] = value
        for r, dev in ((1, nb_c), (2, nb_x), (3, nb_xc)):
            remote(sums.at[it, 0, :, pl.ds(lo, width)], sums.at[it, r, :, pl.ds(lo, width)],
                   ar_s, ar_r.at[index], dev).start()
        return it, lo, width, index

    def three(it, lo, width, index):
        at = sums.at[it, pl.ds(1, 3), :, pl.ds(lo, width)]
        return remote(at, at, ar_s, ar_r.at[index], nb_c)

    def gathered(handle):
        it, lo, width, index = handle
        three(it, lo, width, index).wait_recv()
        s = [sums[it, r, :, lo:lo + width] for r in range(4)]
        return float(ORDER) / ((s[0] + s[1]) + (s[2] + s[3]))

    def square_and_share(it, dst, lo, width, value):
        m = value * value
        dst[:, lo:lo + width] = m
        return share(it, lo, width, jnp.sum(m, axis=0, keepdims=True))

    def rescale(dst, src, handle):
        f = gathered(handle)
        lo, width = handle[1:3]
        dst[:, lo:lo + width] = (src[:, lo:lo + width] * f).astype(BF16)

    def graph(lo, depth, first, width):
        return G[first // COLS, lo:lo + depth, first % COLS:first % COLS + width]

    def far_piece(i):
        dx_cp[i].wait_recv()
        c3_cp[i].start()

    bytes_of(3 * ROWS - LENT, snd.at[0], c2_r).wait_send()
    shared = []
    for n in range(NKC):
        if n < NKC - 1:
            bytes_of(2 * SUB, snd.at[0], far_r.at[n]).wait_recv()
            c3_cp[n].start()
        else:
            far_piece(n)
        for i in ((2,), (3, 4), (), ())[n]:
            dx_cp[i].start()
        if n + 2 < NKC:
            ay_cp[n + 2].start()
        if n == 2:
            bytes_of(2 * ROWS - LENT, snd.at[1], c2_r).wait_send()

            @pl.when(core == 1)
            def _():
                bytes_of(4 * LENT, snd.at[3], c2_r).wait_send()

        if n == NKC - 1:

            @pl.when(core == 1)
            def _():
                far_piece(NSUB)

            ay_cp[n].wait_recv()
        lo = KC * n
        hi = COLS + lo
        if n < NKC - 1:
            C1[:, :COLS] += dot(A0[:, hi:hi + KC], G[0, hi:hi + KC, :])
        else:
            for first, width in PIECES_1:
                if first < COLS:
                    v = C1[:, first:first + width] + dot(A0[:, hi:hi + KC], graph(hi, KC, first, width))
                    shared.append(square_and_share(0, C1, first, width, v))
                    if len(shared) == 1:

                        @pl.when(core == 0)
                        def _():
                            far_piece(NSUB)

        if n < 2:
            continue
        bytes_of(SUB * (3 if n == 2 else 1), snd.at[0], c3_r.at[n - 2]).wait_recv()
        for first, width in PIECES_1:
            if first < COLS:
                continue
            if n == 2:
                C1[:, first:first + width] = (dot(A0[:, :hi - COLS + KC], graph(0, lo + KC, first, width))
                                              + dot(A0[:, COLS:hi + KC], graph(COLS, lo + KC, first, width)))
            else:
                d = dot(A0[:, lo:lo + KC], graph(lo, KC, first, width)) + dot(A0[:, hi:hi + KC], graph(hi, KC, first, width))
                shared.append(square_and_share(0, C1, first, width, C1[:, first:first + width] + d))

    bytes_of(2 * ROWS, snd.at[2], c2_r).wait_send()
    bytes_of(ROWS, snd.at[0], c2_r).wait_send()
    lo, depth = PIECES_1[0]
    a = (C1[:, lo:lo + depth] * gathered(shared[0])).astype(BF16)
    for hc in range(2):
        C2[:, hc * COLS:(hc + 1) * COLS] = dot(a, G[hc, lo:lo + depth, :])
    rescale(A1, C1, shared[1])
    lo, depth = PIECES_1[1]
    for first, width in PIECES_2[:EARLY]:
        C2[:, first:first + width] += dot(A1[:, lo:lo + depth], graph(lo, depth, first, width))
    f = gathered(shared[2])
    three(0, 0, ORDER, 0).wait_send()
    shared = []
    held = None
    for t, (first, width) in enumerate(PIECES_2):
        v = C2[:, first:first + width]
        for lo, depth in PIECES_1[2 if t < EARLY else 1:]:
            for at in range(lo, lo + depth, STEP):
                if t == 0:
                    A1[:, at:at + STEP] = (C1[:, at:at + STEP] * f[:, at - lo:at - lo + STEP]).astype(BF16)
                v += dot(A1[:, at:at + STEP], graph(at, STEP, first, width))
                if held is not None:
                    shared.append(share(1, *held))
                    held = None
        m = v * v
        C2[:, first:first + width] = m
        held = first, width, jnp.sum(m, axis=0, keepdims=True)
    shared.append(share(1, *held))

    for t, (lo, depth) in enumerate(PIECES_2):
        if t == len(PIECES_2) - 1:
            three(1, 0, ORDER, 0).wait_send()
        f = gathered(shared[t])
        d = dot((C2[:, lo:lo + depth] * f).astype(BF16), G[0, lo:lo + depth, :])
        if t == 0:
            C1[:, :COLS] = d
        elif t < len(PIECES_2) - 1:
            C1[:, :COLS] += d
        else:
            v = C1[:, :COLS] + d
            m = v * v
            last = share(2, 0, COLS, jnp.sum(m, axis=0, keepdims=True))
            for b in range(8):
                p = place(b)
                m_ref[:, 128 * b:128 * b + 128] = m[:, 128 * p:128 * p + 128]
    f = gathered(last)
    for b in range(8):
        p = place(b)
        r_ref[:, 128 * b:128 * b + 128] = f[:, 128 * p:128 * p + 128]
    three(2, 0, COLS, 0).wait_send()


def scale_kernel(m_ref, r_ref, out_hbm, out, sem):
    factor = r_ref[...]
    step = ROWS // 16
    for i in range(16):
        at = pl.ds(step * i, step)
        out[at, :] = m_ref[at, :] * factor
        pltpu.make_async_copy(out.at[at], out_hbm.at[at], sem).start()
    pltpu.make_async_copy(out, out_hbm, sem).wait()


def solution(mesh):
    block_spec = P(("graph", "row"), "col")

    def device_step(init_blk, graph_blk):
        dma = pltpu.SemaphoreType.DMA
        in_hbm = [pltpu.with_memory_space_constraint(v, pltpu.HBM) for v in (init_blk, graph_blk)]
        m, r = pl.pallas_call(
            mcl_kernel,
            name="mcl",
            out_shape=(jax.ShapeDtypeStruct((ROWS, COLS), F32), jax.ShapeDtypeStruct((1, COLS), F32)),
            in_specs=[pl.BlockSpec(memory_space=pltpu.HBM)] * 2,
            out_specs=(pl.BlockSpec(memory_space=pltpu.VMEM),) * 2,
            scratch_shapes=[
                pltpu.VMEM((ROWS, COLS), F32),
                pltpu.VMEM((ROWS, COLS), F32),
                pltpu.VMEM((2, ORDER, COLS), BF16),
                pltpu.VMEM((ROWS, ORDER), BF16),
                pltpu.VMEM((ROWS, ORDER), BF16),
                pltpu.VMEM((ROWS, ORDER), F32),
                pltpu.VMEM((ROWS, ORDER), F32),
                pltpu.VMEM((3, 4, 1, ORDER), F32),
                dma((4,)), dma((4,)), dma((3,)), dma((NSUB + 2,)),
                dma(()), dma(()), dma(()), dma(()), dma((2,)),
                dma(()), dma((len(PIECES_1) + len(PIECES_2) + 1,)),
            ],
            compiler_params=pltpu.CompilerParams(collective_id=0, has_side_effects=True, vmem_limit_bytes=48 * 2**20),
        )(*in_hbm)
        return pl.pallas_call(
            scale_kernel,
            name="scale",
            out_shape=jax.ShapeDtypeStruct((ROWS, COLS), F32),
            in_specs=[pl.BlockSpec(memory_space=pltpu.VMEM)] * 2,
            out_specs=pl.BlockSpec(memory_space=pltpu.HBM),
            scratch_shapes=[pltpu.VMEM((ROWS, COLS), F32), dma(())],
            compiler_params=pltpu.CompilerParams(vmem_limit_bytes=8 * 2**20),
        )(m, r)

    return jax.shard_map(device_step, mesh=mesh, in_specs=(block_spec, block_spec), out_specs=block_spec, check_vma=False)
```

```python
import jax
import jax.numpy as jnp
from jax import lax
from jax.experimental import pallas as pl
from jax.experimental.pallas import tpu as pltpu
from jax.sharding import PartitionSpec as P

MESH = pl.DeviceIdType.MESH
BF16 = jnp.bfloat16
F32 = jnp.float32

ROWS = 512
COLS = 1024
ORDER = 2048
SUB = 128
NSUB = ROWS // SUB
HALF = SUB // 2
FIRST = 32
LENT = 48
TAIL = (NSUB - 1, NSUB - 0.5)
KC = 256
NKC = COLS // KC
PIECES_1 = ((0, 512), (512, 512), (1024, 1024))
EARLY = 1
STEP = 512
PIECES_2 = ((1024, 512), (1536, 512), (0, 512), (512, 512))


def place(b):
    return 2 * (b % 4) + b // 4


def mcl_kernel(a_hbm, g_hbm, m_ref, r_ref,
               a_f32, g_f32, G, A0, A1, C1, C2, sums,
               ld_sem, snd, in_r, far_r, c0_r, c01_r, c2_r, c2x_r, c3_r, ar_s, ar_r):
    graph, col, row = lax.axis_index("graph"), lax.axis_index("col"), lax.axis_index("row")
    x, core = row // 2, row % 2
    nb_x = (graph, col, (1 - x) * 2 + core)
    nb_y = (graph, 1 - col, row)
    nb_c = (graph, col, x * 2 + 1 - core)
    nb_xc = (graph, col, (1 - x) * 2 + 1 - core)

    half_own = lax.rem(x + col, 2)
    half_far = 1 - half_own

    def position(half, side, sub):
        return pl.multiple_of(half * COLS + KC * (int(sub)) + SUB * side + int(SUB * (sub % 1)), HALF)

    def remote(ref_src, ref_dst, send, recv, dev):
        return pltpu.make_async_remote_copy(src_ref=ref_src, dst_ref=ref_dst, send_sem=send, recv_sem=recv,
                                            device_id=dev, device_id_type=MESH)

    cuts = (0, FIRST, 2 * FIRST, ROWS)
    loads = [pltpu.make_async_copy(g_hbm.at[pl.ds(lo, hi - lo)], g_f32.at[pl.ds(lo, hi - lo)], ld_sem.at[i])
             for i, (lo, hi) in enumerate(zip(cuts, cuts[1:]))]
    loads.append(pltpu.make_async_copy(a_hbm, a_f32, ld_sem.at[len(loads)]))
    for cp in loads:
        cp.start()

    barrier = pltpu.get_barrier_semaphore()
    for dev in (nb_x, nb_y, nb_c):
        pl.semaphore_signal(barrier, inc=1, device_id=dev, device_id_type=MESH)

    def rows(hc, half, side, sub, n=SUB):
        return G.at[hc, pl.ds(position(half, side, sub), n)]

    own_at = [rows(0, half_own, core, i) for i in range(NSUB)]
    gx_at = [rows(0, half_far, core, i) for i in range(NSUB)]
    gy_at = [rows(1, half_own, core, i) for i in range(NSUB)]
    dx_at = [rows(1, half_far, core, i) for i in range(NSUB)]
    tail_y = [rows(1, half_own, core, i, HALF) for i in TAIL]
    tail_d = [rows(1, half_far, core, i, HALF) for i in TAIL]

    gx_cp = [remote(own_at[i], own_at[i], snd.at[0], in_r.at[i // 2], nb_x) for i in range(NSUB)]
    def last_rows(hc, half, extra):
        first = half * COLS + KC * (NSUB - 1)
        if extra:
            return G.at[hc, pl.ds(pl.multiple_of(first + 2 * (SUB - LENT), 16), 2 * LENT)]
        return G.at[hc, pl.ds(pl.multiple_of(first + (SUB - LENT) * core, 16), SUB - LENT)]

    gy_cp = [remote(own_at[i], dx_at[i], snd.at[0], in_r.at[i // 2], nb_y) for i in range(NSUB - 1)]
    gy_cp += [remote(last_rows(0, half_own, e), last_rows(1, half_far, e), snd.at[3 if e else 0], in_r.at[1 + e], nb_y)
              for e in range(2)]
    dx_cp = [remote(at, at, snd.at[2], far_r.at[i], nb_x) for i, at in enumerate(gy_at[:-1] + tail_y)]
    c0_cp = [remote(at, at, snd.at[0], c0_r if i == NSUB - 1 else c01_r, nb_c) for i, at in enumerate(own_at)]
    c1_cp = [remote(at, at, snd.at[1], c01_r, nb_c) for at in gx_at]
    c2_cp = [remote(at, at, snd.at[1], c2_r, nb_c) for at in gy_at[:-1]]
    c2_cp += [remote(last_rows(1, half_own, e), last_rows(1, half_own, e), snd.at[3 if e else 1], c2x_r if e else c2_r, nb_c)
              for e in range(2)]
    c3_cp = [remote(at, at, snd.at[0], c3_r.at[0 if i < NSUB - 1 else 1], nb_c) for i, at in enumerate(dx_at[:-1] + tail_d)]
    ay_cp = [remote(A0.at[:, pl.ds(KC * n, KC)], A0.at[:, pl.ds(COLS + KC * n, KC)], snd.at[2], far_r.at[n if n < NKC - 1 else NSUB + 1], nb_y)
             for n in range(NKC)]

    def bytes_of(count, send, recv):
        at = G.at[0, pl.ds(0, count)] if count <= ORDER else G.at[:, pl.ds(0, count // 2)]
        return remote(at, at, send, recv, nb_c)

    def send_own(lo, hi):
        i = lo // SUB
        if hi - lo == SUB:
            gx_cp[i].start()
            if i < NSUB - 1:
                gy_cp[i].start()
            c0_cp[i].start()
        else:
            at = G.at[0, pl.ds(pl.multiple_of(position(half_own, core, 0) + lo, FIRST), hi - lo)]
            there = G.at[1, pl.ds(pl.multiple_of(position(half_far, core, 0) + lo, FIRST), hi - lo)]
            remote(at, at, snd.at[0], in_r.at[0], nb_x).start()
            remote(at, there, snd.at[0], in_r.at[0], nb_y).start()
            remote(at, at, snd.at[0], c01_r, nb_c).start()

    parts = (*zip((0, FIRST, 2 * FIRST), (FIRST, 2 * FIRST, SUB)), *((SUB * i, SUB * (i + 1)) for i in range(1, NSUB)))
    for t, (lo, hi) in enumerate(parts):
        if lo in cuts:
            loads[cuts.index(lo)].wait()
        for b in range(8):
            p = place(b)
            G[0, pl.ds(pl.multiple_of(position(half_own, core, lo // SUB) + lo % SUB, FIRST), hi - lo), 128 * p:128 * p + 128] = (
                g_f32[lo:hi, 128 * b:128 * b + 128].astype(BF16))
        if t == 0:
            pl.semaphore_wait(barrier, 3)
        else:
            send_own(*parts[t - 1])
    loads[-1].wait()
    for b in range(8):
        p = place(b)
        A0[:, 128 * p:128 * p + 128] = a_f32[:, 128 * b:128 * b + 128].astype(BF16)
    send_own(*parts[-1])

    def dot(a, g):
        return jnp.dot(a, g, preferred_element_type=F32)

    c0_cp[-1].wait_recv()
    gy_cp[NSUB - 1].start()

    @pl.when(core == 1)
    def _():
        gy_cp[NSUB].start()

    for half in range(2):
        bytes_of(4 * SUB - half * LENT, snd.at[0], in_r.at[half]).wait_recv()
        for i in (2 * half, 2 * half + 1):
            c1_cp[i].start()
            c2_cp[i].start()
        if half == 0:
            for i in range(2):
                dx_cp[i].start()
                ay_cp[i].start()

    @pl.when(core == 1)
    def _():
        gy_cp[NSUB].wait_recv()
        c2_cp[NSUB].start()

    bytes_of(7 * SUB, snd.at[0], c01_r).wait_recv()
    C1[:, :COLS] = dot(A0[:, :COLS], G[0, :COLS, :])
    bytes_of(ROWS - LENT, snd.at[1], c2_r).wait_recv()

    @pl.when(core == 0)
    def _():
        c2_cp[NSUB].wait_recv()

    slots = []

    def share(it, lo, width, value):
        index = len(slots)
        slots.append(index)
        sums[it, 0, :, lo:lo + width] = value
        for r, dev in ((1, nb_c), (2, nb_x), (3, nb_xc)):
            remote(sums.at[it, 0, :, pl.ds(lo, width)], sums.at[it, r, :, pl.ds(lo, width)],
                   ar_s, ar_r.at[index], dev).start()
        return it, lo, width, index

    def three(it, lo, width, index):
        at = sums.at[it, pl.ds(1, 3), :, pl.ds(lo, width)]
        return remote(at, at, ar_s, ar_r.at[index], nb_c)

    def gathered(handle):
        it, lo, width, index = handle
        three(it, lo, width, index).wait_recv()
        s = [sums[it, r, :, lo:lo + width] for r in range(4)]
        return float(ORDER) / ((s[0] + s[1]) + (s[2] + s[3]))

    def square_and_share(it, dst, lo, width, value):
        m = value * value
        dst[:, lo:lo + width] = m
        return share(it, lo, width, jnp.sum(m, axis=0, keepdims=True))

    def rescale(dst, src, handle):
        f = gathered(handle)
        lo, width = handle[1:3]
        dst[:, lo:lo + width] = (src[:, lo:lo + width] * f).astype(BF16)

    def graph(lo, depth, first, width):
        return G[first // COLS, lo:lo + depth, first % COLS:first % COLS + width]

    def far_piece(i):
        dx_cp[i].wait_recv()
        c3_cp[i].start()

    bytes_of(3 * ROWS - LENT, snd.at[0], c2_r).wait_send()
    shared = []
    for n in range(NKC):
        if n < NKC - 1:
            bytes_of(2 * SUB, snd.at[0], far_r.at[n]).wait_recv()
            c3_cp[n].start()
        else:
            far_piece(n)
        for i in ((2,), (3, 4), (), ())[n]:
            dx_cp[i].start()
        if n + 2 < NKC:
            ay_cp[n + 2].start()
        if n == 2:
            bytes_of(2 * ROWS - LENT, snd.at[1], c2_r).wait_send()

            @pl.when(core == 1)
            def _():
                bytes_of(4 * LENT, snd.at[3], c2_r).wait_send()

        if n == NKC - 1:

            @pl.when(core == 1)
            def _():
                far_piece(NSUB)

            ay_cp[n].wait_recv()
        lo = KC * n
        hi = COLS + lo
        if n < NKC - 1:
            C1[:, :COLS] += dot(A0[:, hi:hi + KC], G[0, hi:hi + KC, :])
        else:
            for first, width in PIECES_1:
                if first < COLS:
                    v = C1[:, first:first + width] + dot(A0[:, hi:hi + KC], graph(hi, KC, first, width))
                    shared.append(square_and_share(0, C1, first, width, v))
                    if len(shared) == 1:

                        @pl.when(core == 0)
                        def _():
                            far_piece(NSUB)

        if n < 2:
            continue
        bytes_of(SUB * (3 if n == 2 else 1), snd.at[0], c3_r.at[n - 2]).wait_recv()
        for first, width in PIECES_1:
            if first < COLS:
                continue
            if n == 2:
                C1[:, first:first + width] = (dot(A0[:, :hi - COLS + KC], graph(0, lo + KC, first, width))
                                              + dot(A0[:, COLS:hi + KC], graph(COLS, lo + KC, first, width)))
            else:
                d = dot(A0[:, lo:lo + KC], graph(lo, KC, first, width)) + dot(A0[:, hi:hi + KC], graph(hi, KC, first, width))
                shared.append(square_and_share(0, C1, first, width, C1[:, first:first + width] + d))

    bytes_of(2 * ROWS, snd.at[2], c2_r).wait_send()
    bytes_of(ROWS, snd.at[0], c2_r).wait_send()
    lo, depth = PIECES_1[0]
    a = (C1[:, lo:lo + depth] * gathered(shared[0])).astype(BF16)
    for hc in range(2):
        C2[:, hc * COLS:(hc + 1) * COLS] = dot(a, G[hc, lo:lo + depth, :])
    rescale(A1, C1, shared[1])
    lo, depth = PIECES_1[1]
    for first, width in PIECES_2[:EARLY]:
        C2[:, first:first + width] += dot(A1[:, lo:lo + depth], graph(lo, depth, first, width))
    f = gathered(shared[2])
    three(0, 0, ORDER, 0).wait_send()
    shared = []
    held = None
    for t, (first, width) in enumerate(PIECES_2):
        v = C2[:, first:first + width]
        for lo, depth in PIECES_1[2 if t < EARLY else 1:]:
            for at in range(lo, lo + depth, STEP):
                if t == 0:
                    A1[:, at:at + STEP] = (C1[:, at:at + STEP] * f[:, at - lo:at - lo + STEP]).astype(BF16)
                v += dot(A1[:, at:at + STEP], graph(at, STEP, first, width))
                if held is not None:
                    shared.append(share(1, *held))
                    held = None
        m = v * v
        C2[:, first:first + width] = m
        held = first, width, jnp.sum(m, axis=0, keepdims=True)
    shared.append(share(1, *held))

    for t, (lo, depth) in enumerate(PIECES_2):
        if t == len(PIECES_2) - 1:
            three(1, 0, ORDER, 0).wait_send()
        f = gathered(shared[t])
        d = dot((C2[:, lo:lo + depth] * f).astype(BF16), G[0, lo:lo + depth, :])
        if t == 0:
            C1[:, :COLS] = d
        elif t < len(PIECES_2) - 1:
            C1[:, :COLS] += d
        else:
            v = C1[:, :COLS] + d
            m = v * v
            last = share(2, 0, COLS, jnp.sum(m, axis=0, keepdims=True))
            for b in range(8):
                p = place(b)
                m_ref[:, 128 * b:128 * b + 128] = m[:, 128 * p:128 * p + 128]
    f = gathered(last)
    for b in range(8):
        p = place(b)
        r_ref[:, 128 * b:128 * b + 128] = f[:, 128 * p:128 * p + 128]
    three(2, 0, COLS, 0).wait_send()


def scale_kernel(m_ref, r_ref, out_hbm, out, sem):
    factor = r_ref[...]
    step = ROWS // 16
    for i in range(16):
        at = pl.ds(step * i, step)
        out[at, :] = m_ref[at, :] * factor
        pltpu.make_async_copy(out.at[at], out_hbm.at[at], sem).start()
    pltpu.make_async_copy(out, out_hbm, sem).wait()


def solution(mesh):
    block_spec = P(("graph", "row"), "col")

    def device_step(init_blk, graph_blk):
        dma = pltpu.SemaphoreType.DMA
        in_hbm = [pltpu.with_memory_space_constraint(v, pltpu.HBM) for v in (init_blk, graph_blk)]
        m, r = pl.pallas_call(
            mcl_kernel,
            name="mcl",
            out_shape=(jax.ShapeDtypeStruct((ROWS, COLS), F32), jax.ShapeDtypeStruct((1, COLS), F32)),
            in_specs=[pl.BlockSpec(memory_space=pltpu.HBM)] * 2,
            out_specs=(pl.BlockSpec(memory_space=pltpu.VMEM),) * 2,
            scratch_shapes=[
                pltpu.VMEM((ROWS, COLS), F32),
                pltpu.VMEM((ROWS, COLS), F32),
                pltpu.VMEM((2, ORDER, COLS), BF16),
                pltpu.VMEM((ROWS, ORDER), BF16),
                pltpu.VMEM((ROWS, ORDER), BF16),
                pltpu.VMEM((ROWS, ORDER), F32),
                pltpu.VMEM((ROWS, ORDER), F32),
                pltpu.VMEM((3, 4, 1, ORDER), F32),
                dma((4,)), dma((4,)), dma((3,)), dma((NSUB + 2,)),
                dma(()), dma(()), dma(()), dma(()), dma((2,)),
                dma(()), dma((len(PIECES_1) + len(PIECES_2) + 1,)),
            ],
            compiler_params=pltpu.CompilerParams(collective_id=0, has_side_effects=True, vmem_limit_bytes=48 * 2**20),
        )(*in_hbm)
        return pl.pallas_call(
            scale_kernel,
            name="scale",
            out_shape=jax.ShapeDtypeStruct((ROWS, COLS), F32),
            in_specs=[pl.BlockSpec(memory_space=pltpu.VMEM)] * 2,
            out_specs=pl.BlockSpec(memory_space=pltpu.HBM),
            scratch_shapes=[pltpu.VMEM((ROWS, COLS), F32), dma(())],
            compiler_params=pltpu.CompilerParams(vmem_limit_bytes=8 * 2**20),
        )(m, r)

    return jax.shard_map(device_step, mesh=mesh, in_specs=(block_spec, block_spec), out_specs=block_spec, check_vma=False)
```
